128 devices in a mesh: dp: 1, tp: 16 (over z, y), cp: 8 (over x, core).
Axes of the slice: x: 4, y: 4, z: 4, core: 2. Of those that a mesh axis runs over, the one named last changes fastest.
Arguments:
- x: bfloat16 [4096, 8192], P(('dp', 'cp'))
- doc_ids: int32 [4096], P(('dp', 'cp'))
- w_query: bfloat16 [8192, 8192], P(None, 'tp')
- w_key: bfloat16 [8192, 8192], P(None, 'tp')
- w_value: bfloat16 [8192, 8192], P(None, 'tp')
- w_out: bfloat16 [8192, 8192], P('tp')
Outputs:
- output: bfloat16 [4096, 8192], P(('dp', 'cp'))
All inputs are finite; a program needn't handle non-finite values.
Results may differ from the reference program's by a relative error of at most 0.0071832.
Values are sent between devices in bfloat16 or wider.
A program may use at most 1 GiB of HBM per device.

```python
import jax
import jax.numpy as jnp
from jax import lax

SEQ_LEN = 4096
BLOCK_LEN = 256
DOC_BREAKS = 32
D = 8192
HEADS = 64
KV_HEADS = 64
HEAD = 128


def setup_inputs(seed: int = 0, part: int = 0) -> dict:
    shared_keys = jax.random.split(jax.random.key(seed), 4)
    part_keys = jax.random.split(jax.random.fold_in(jax.random.key(seed + 1), part), 4)
    x = jax.random.normal(part_keys[0], (SEQ_LEN, D), jnp.float32).astype(jnp.bfloat16)
    span_len = jax.random.randint(part_keys[1], (), SEQ_LEN // 3, 2 * SEQ_LEN // 3 + 1)
    span_start = jax.random.randint(part_keys[2], (), 0, SEQ_LEN - span_len + 1)
    breaks = jax.random.randint(part_keys[3], (DOC_BREAKS,), 1, SEQ_LEN)
    inside = (breaks > span_start) & (breaks < span_start + span_len)
    start_flags = jnp.zeros((SEQ_LEN,), jnp.int32).at[breaks].add(jnp.where(inside, 0, 1))
    doc_ids = jnp.cumsum(start_flags).astype(jnp.int32)
    w_query = (jax.random.normal(shared_keys[0], (D, HEADS * HEAD), jnp.float32) * (1.5 / D ** 0.5)).astype(jnp.bfloat16)
    w_key = (jax.random.normal(shared_keys[1], (D, KV_HEADS * HEAD), jnp.float32) * (1.5 / D ** 0.5)).astype(jnp.bfloat16)
    w_value = (jax.random.normal(shared_keys[2], (D, KV_HEADS * HEAD), jnp.float32) / D ** 0.5).astype(jnp.bfloat16)
    w_out = (jax.random.normal(shared_keys[3], (HEADS * HEAD, D), jnp.float32) * (2.0 / (HEADS * HEAD) ** 0.5)).astype(jnp.bfloat16)
    return {'x': x, 'doc_ids': doc_ids, 'w_query': w_query, 'w_key': w_key, 'w_value': w_value, 'w_out': w_out}


def block_update(soft_state, q_blk, k_blk, v_blk, allowed):
    run_max, run_sum, out_acc = soft_state
    scores = jnp.einsum('qhgd,khd->qhgk', q_blk.astype(jnp.float32), k_blk.astype(jnp.float32)) * (HEAD ** -0.5)
    scores = jnp.where(allowed[:, None, None, :], scores, -jnp.inf)
    new_max = jnp.maximum(run_max, jnp.max(scores, axis=-1))
    safe_max = jnp.where(new_max == -jnp.inf, 0.0, new_max)
    prob_vals = jnp.exp(scores - safe_max[..., None])
    rescale = jnp.exp(run_max - safe_max)
    run_sum = run_sum * rescale + jnp.sum(prob_vals, axis=-1)
    out_acc = out_acc * rescale[..., None] + jnp.einsum('qhgk,khd->qhgd', prob_vals, v_blk.astype(jnp.float32))
    return new_max, run_sum, out_acc


def reference(x, doc_ids, w_query, w_key, w_value, w_out):
    q_per_kv = HEADS // KV_HEADS
    n_blocks = SEQ_LEN // BLOCK_LEN
    q_all = jnp.dot(x, w_query, preferred_element_type=jnp.float32).astype(jnp.bfloat16).reshape(n_blocks, BLOCK_LEN, KV_HEADS, q_per_kv, HEAD)
    k_all = jnp.dot(x, w_key, preferred_element_type=jnp.float32).astype(jnp.bfloat16).reshape(n_blocks, BLOCK_LEN, KV_HEADS, HEAD)
    v_all = jnp.dot(x, w_value, preferred_element_type=jnp.float32).astype(jnp.bfloat16).reshape(n_blocks, BLOCK_LEN, KV_HEADS, HEAD)
    seg_blocks = doc_ids.reshape(n_blocks, BLOCK_LEN)
    pos_blocks = jnp.arange(SEQ_LEN).reshape(n_blocks, BLOCK_LEN)

    def query_block(q_inputs):
        q_blk, seg_q, pos_q = q_inputs

        def key_step(soft_state, k_inputs):
            k_blk, v_blk, seg_k, pos_k = k_inputs
            active = (pos_k[0] <= pos_q[BLOCK_LEN - 1]) & (seg_k[BLOCK_LEN - 1] >= seg_q[0])
            allowed = (seg_q[:, None] == seg_k[None, :]) & (pos_q[:, None] >= pos_k[None, :])
            new_state = lax.cond(active, lambda same_state: block_update(same_state, q_blk, k_blk, v_blk, allowed), lambda same_state: same_state, soft_state)
            return new_state, None

        init_state = (jnp.full((BLOCK_LEN, KV_HEADS, q_per_kv), -jnp.inf, jnp.float32), jnp.zeros((BLOCK_LEN, KV_HEADS, q_per_kv), jnp.float32), jnp.zeros((BLOCK_LEN, KV_HEADS, q_per_kv, HEAD), jnp.float32))
        final_state = lax.scan(key_step, init_state, (k_all, v_all, seg_blocks, pos_blocks))[0]
        run_sum = final_state[1]
        out_acc = final_state[2]
        return (out_acc / run_sum[..., None]).astype(jnp.bfloat16).reshape(BLOCK_LEN, HEADS * HEAD)

    heads_out = lax.map(query_block, (q_all, seg_blocks, pos_blocks)).reshape(SEQ_LEN, HEADS * HEAD)
    return jnp.dot(heads_out, w_out, preferred_element_type=jnp.float32).astype(jnp.bfloat16)
```

```python
import jax
import jax.numpy as jnp
from jax import lax
from jax.experimental import pallas as pl
from jax.experimental.pallas import tpu as pltpu
from jax.sharding import PartitionSpec as P

MESH = pl.DeviceIdType.MESH
HD = 128
NX = 4
L = 512
D = 8192
F = 512
KC = 1024
NKC = D // KC
NB = 4
PRE = 3
R = 4
RL = L // R
QT = 256
SCALE = (HD ** -0.5) * 1.4426950408889634
BF = jnp.bfloat16
F32 = jnp.float32


def mod(a, n):
    return lax.rem(a + n, n)


def kernel(x_hbm, seg_hbm, wq_hbm, wk_hbm, wv_hbm, wo_hbm, y_hbm,
           xbuf, wbuf, acc, kloc, vloc, qloc, kg, vg, qg, obuf, og, wt, psend, pown, rsb, yg, segs, sq, m_s, l_s, o_s,
           x_sem, w_sem, wo_sem, ws_send, ws_recv, wf_send, wf_recv,
           kv_send, kv_recv, kf_send, kf_recv, q_send, q_recv, o_send, o_recv,
           sg_send, sg_recv, sg_loc, a_send, a_recv, r_send, r_recv, y_send, y_recv, out_sem):
    t = lax.axis_index("tp")
    c = lax.axis_index("cp")
    x, k = c // 2, lax.rem(c, 2)
    z, y = t // NX, lax.rem(t, NX)
    yh, yb = y // 2, lax.rem(y, 2)
    xodd = lax.rem(x, 2)
    partner = {"cp": x * 2 + 1 - k}

    def iy(yy):
        return lax.rem(yy + yy // 2, 2)

    def slice_of(zz, yy):
        return zz * 2 + iy(yy)

    def piece_of(zz, yy):
        return slice_of(zz, yy) * 2 + yy // 2

    def tpdev(zz, yy):
        return {"tp": zz * NX + yy}

    def rcopy(src, dst, ss, rs, dev):
        return pltpu.make_async_remote_copy(src_ref=src, dst_ref=dst, send_sem=ss, recv_sem=rs, device_id=dev, device_id_type=MESH)

    s_me = z * 2 + yb
    sl_me = slice_of(z, y)
    sends = []

    def x_copy(i):
        return pltpu.make_async_copy(x_hbm.at[:, pl.ds(pl.multiple_of(i * KC, KC), KC)], xbuf.at[i], x_sem.at[i])

    w_hbms = (wk_hbm, wv_hbm, wq_hbm)

    def w_copy(w, i):
        slot = lax.rem(i, NB)
        return pltpu.make_async_copy(w_hbms[w].at[pl.ds(pl.multiple_of(i * KC, KC), KC), :], wbuf.at[slot], w_sem.at[slot])

    for i in range(PRE):
        x_copy(jnp.int32(i)).start()
        w_copy(0, jnp.int32(i)).start()
    seg_own = pltpu.make_async_copy(seg_hbm, segs.at[c], sg_loc)
    seg_own.start()
    wo_own = pltpu.make_async_copy(wo_hbm.at[:, pl.ds(pl.multiple_of(sl_me * 1024, 1024), 1024)],
                                   wt.at[pl.ds(pl.multiple_of(s_me * F, F), F), :], wo_sem)

    bar = pltpu.get_barrier_semaphore()
    n_peers = 0
    for dc in range(1, 2 * NX):
        pl.semaphore_signal(bar, inc=1, device_id={"cp": mod(c + dc, 2 * NX)}, device_id_type=MESH)
        n_peers += 1
    for dz in range(NX):
        for e in range(2):
            if dz or e:
                pl.semaphore_signal(bar, inc=1, device_id=tpdev(mod(z + dz, NX), yh * 2 + lax.rem(yb + e, 2)), device_id_type=MESH)
                n_peers += 1
    pl.semaphore_signal(bar, inc=1, device_id=tpdev(z, 3 - y), device_id_type=MESH)
    n_peers += 1
    pl.semaphore_wait(bar, n_peers)

    def w_move(dz, e):
        z2, y2 = mod(z + dz, NX), yh * 2 + lax.rem(yb + e, 2)
        i = dz * 2 + e - 1
        return rcopy(wo_hbm.at[pl.ds(pl.multiple_of(k * 256, 256), 256), pl.ds(pl.multiple_of(slice_of(z2, y2) * 1024, 1024), 1024)],
                     wt.at[pl.ds(pl.multiple_of(s_me * F + k * 256, 256), 256), :],
                     ws_send.at[i], ws_recv.at[i], tpdev(z2, y2))

    def w_rows(dz, e, kk):
        s = mod(z - dz, NX) * 2 + lax.rem(yb + e, 2)
        return wt.at[pl.ds(pl.multiple_of(s * F + kk * 256, 256), 256), :]

    def w_fwd(dz, e, kk):
        i = dz * 2 + e - 1
        ref = w_rows(dz, e, kk)
        return rcopy(ref, ref, wf_send.at[i], wf_recv.at[i], partner)

    group = [(dz, e) for dz in range(NX) for e in range(2) if dz or e]
    seg_own.wait()
    for dc in range(1, 2 * NX):
        cp_ = rcopy(segs.at[c], segs.at[c], sg_send.at[dc - 1], sg_recv.at[dc - 1], {"cp": mod(c + dc, 2 * NX)})
        cp_.start()
        sends.append(cp_)
    for dz, e in group:
        cp_ = w_move(dz, e)
        cp_.start()
        sends.append(cp_)
    wo_own.start()

    def project(w, lo, hi):
        def step(i, _):
            nxt = i + PRE

            @pl.when(nxt < NKC)
            def _():
                w_copy(w, nxt).start()
                if w == 0:
                    x_copy(nxt).start()
            if w < 2:
                @pl.when(nxt >= NKC)
                def _():
                    w_copy(w + 1, nxt - NKC).start()
            w_copy(w, i).wait()
            if w == 0:
                x_copy(i).wait()
            slot = lax.rem(i, NB)
            acc[...] += jnp.dot(xbuf[i], wbuf[slot], preferred_element_type=F32)
            return 0
        lax.fori_loop(lo, hi, step, 0)

    def split(dst):
        for h in range(4):
            dst[h] = acc[:, h * HD:(h + 1) * HD].astype(BF)

    def kv_spread(n, loc, gat):
        for dx in range(1, NX):
            h = mod(x + dx, NX)
            cp_ = rcopy(loc.at[h], gat.at[c], kv_send.at[n, dx - 1], kv_recv.at[n, dx - 1], {"cp": h * 2 + k})
            cp_.start()
            sends.append(cp_)
        cp_ = rcopy(loc.at[x], gat.at[c], kv_send.at[n, 3], kv_recv.at[n, 3], partner)
        cp_.start()
        sends.append(cp_)
        gat[c] = loc[x]

    def kv_forward(n, gat):
        for dx in (1, 3, 2):
            ref = gat.at[mod(x - dx, NX) * 2 + k]
            rcopy(ref, ref, kv_send.at[n, dx - 1], kv_recv.at[n, dx - 1], partner).wait_recv()
            cp_ = rcopy(ref, ref, kf_send.at[n, dx - 1], kf_recv.at[n, dx - 1], partner)
            cp_.start()
            sends.append(cp_)

    def kv_finish(n, gat):
        ref = gat.at[x * 2 + 1 - k]
        rcopy(ref, ref, kv_send.at[n, 3], kv_recv.at[n, 3], partner).wait_recv()
        for dx in (1, 3, 2):
            ref = gat.at[mod(x - dx, NX) * 2 + 1 - k]
            rcopy(ref, ref, kf_send.at[n, dx - 1], kf_recv.at[n, dx - 1], partner).wait_recv()

    acc[...] = jnp.zeros_like(acc)
    project(0, 0, NKC)
    split(kloc)
    acc[...] = jnp.zeros_like(acc)
    kv_spread(0, kloc, kg)
    project(1, 0, NKC)
    split(vloc)
    acc[...] = jnp.zeros_like(acc)
    kv_spread(1, vloc, vg)
    project(2, 0, NKC // 2)
    kv_forward(0, kg)
    project(2, NKC // 2, NKC)
    split(qloc)
    own = lax.rem(x + k, 2)
    for dx in (2, 1, 3):
        h = mod(x + dx, NX)
        cp_ = rcopy(qloc.at[h], qg.at[x], q_send.at[dx - 1], q_recv.at[x], {"cp": h * 2 + own})
        cp_.start()
        sends.append(cp_)

    @pl.when(xodd == 0)
    def _():
        qg[x] = qloc[x]

    q_d2d = rcopy(qloc.at[x], qg.at[x], q_send.at[3], q_recv.at[x], partner)

    @pl.when(xodd == 1)
    def _():
        q_d2d.start()

    kv_forward(1, vg)

    kv_finish(0, kg)
    kv_finish(1, vg)
    for dc in range(1, 2 * NX):
        ref = segs.at[mod(c - dc, 2 * NX)]
        rcopy(ref, ref, sg_send.at[dc - 1], sg_recv.at[dc - 1], partner).wait_recv()

    for xx in range(NX):
        c_q = 2 * xx + lax.rem(k + xx, 2)
        local = (x == xx) & (xodd == 0)

        @pl.when(jnp.logical_not(local))
        def _():
            rcopy(qg.at[xx], qg.at[xx], q_send.at[3], q_recv.at[xx], partner).wait_recv()

        sq[...] = jnp.transpose(jnp.broadcast_to(segs[c_q][0:1, :], (HD, L)))

        for qt in range(L // QT):
            rows = slice(qt * QT, (qt + 1) * QT)
            q_t = qg[xx, rows, :]
            sq_t = jnp.concatenate([sq[rows, :]] * (L // HD), axis=1)

            def scores(j):
                s = lax.dot_general(q_t, kg[j], (((1,), (1,)), ((), ())), preferred_element_type=F32) * SCALE
                return s, sq_t == jnp.broadcast_to(segs[j][0:1, :], (QT, L))

            s, ok = scores(c_q)
            ri = lax.broadcasted_iota(jnp.int32, (QT, L), 0) + qt * QT
            ci = lax.broadcasted_iota(jnp.int32, (QT, L), 1)
            s = jnp.where(ok & (ri >= ci), s, -jnp.inf)
            m0 = jnp.broadcast_to(jnp.max(s, axis=1, keepdims=True), (QT, HD))
            p = jnp.exp2(s - jnp.concatenate([m0] * (L // HD), axis=1))
            m_s[rows, :] = m0
            l_s[rows, :] = jnp.broadcast_to(jnp.sum(p, axis=1, keepdims=True), (QT, HD))
            o_s[rows, :] = jnp.dot(p.astype(BF), vg[c_q], preferred_element_type=F32)

            def kv_step(j, _):
                s, ok = scores(j)
                s = jnp.where(ok, s, -jnp.inf)
                m_old = m_s[rows, :]
                m_new = jnp.maximum(m_old, jnp.max(s, axis=1, keepdims=True))
                alpha = jnp.exp2(m_old - m_new)
                p = jnp.exp2(s - jnp.concatenate([m_new] * (L // HD), axis=1))
                m_s[rows, :] = m_new
                l_s[rows, :] = l_s[rows, :] * alpha + jnp.sum(p, axis=1, keepdims=True)
                o_s[rows, :] = o_s[rows, :] * alpha + jnp.dot(p.astype(BF), vg[j], preferred_element_type=F32)
                return 0
            lax.fori_loop(0, c_q, kv_step, 0)
            obuf[xx, rows, :] = (o_s[rows, :] / l_s[rows, :]).astype(BF)

        ocol = pl.ds(pl.multiple_of(s_me * F + x * HD, HD), HD)
        o_ret = rcopy(obuf.at[xx], og.at[:, ocol], o_send.at[xx], o_recv.at[x], {"cp": c_q})

        @pl.when(local)
        def _():
            og[:, ocol] = obuf[xx]

        @pl.when(jnp.logical_not(local))
        def _():
            o_ret.start()

    for h in range(NX):
        ref = og.at[:, pl.ds(pl.multiple_of(s_me * F + h * HD, HD), HD)]

        @pl.when(jnp.logical_not((x == h) & (xodd == 0)))
        def _():
            rcopy(obuf.at[0], ref, o_send.at[0], o_recv.at[h], partner).wait_recv()

    def o_ref(r, zz, e):
        s = zz * 2 + lax.rem(yb + e, 2)
        return og.at[pl.ds(r * RL, RL), pl.ds(pl.multiple_of(s * F, F), F)]

    def o_copy(r, idx, zz, e, dev):
        ref = o_ref(r, zz, e)
        return rcopy(ref, ref, a_send.at[r, idx], a_recv.at[r, idx], dev)

    def go(cp_):
        cp_.start()
        sends.append(cp_)

    def od(r):
        return 1 if r % 2 == 0 else NX - 1

    def o_send_z(r, e):
        d = od(r)
        go(o_copy(r, 1 + 3 * e, z, e, tpdev(mod(z + d, NX), y)))
        go(o_copy(r, 2 + 3 * e, z, e, tpdev(mod(z + NX - d, NX), y)))

    def o_mid_z(r, e):
        d = od(r)
        zz = mod(z + NX - d, NX)
        o_copy(r, 1 + 3 * e, zz, e, partner).wait_recv()
        go(o_copy(r, 3 + 3 * e, zz, e, tpdev(mod(z + d, NX), y)))

    def o_end_z(r, e):
        d = od(r)
        o_copy(r, 2 + 3 * e, mod(z + d, NX), e, partner).wait_recv()
        o_copy(r, 3 + 3 * e, mod(z + 2, NX), e, partner).wait_recv()

    pair = tpdev(z, yh * 2 + 1 - yb)
    for r in range(R):
        go(o_copy(r, 0, z, 0, pair))
        o_send_z(r, 0)

    for dz, e in group:
        ref = w_rows(dz, e, k)
        i = dz * 2 + e - 1
        rcopy(ref, ref, ws_send.at[i], ws_recv.at[i], partner).wait_recv()
        go(w_fwd(dz, e, k))

    def y_ref(r, zz, yy):
        return yg.at[pl.ds(r * RL, RL), pl.ds(pl.multiple_of(piece_of(zz, yy) * F, F), F)]

    def y_pos(r, a, b):
        if r % 2 == 0:
            return mod(z + a, NX), mod(y + b, NX)
        return mod(z + b, NX), mod(y + a, NX)

    def y_dir(r):
        return (1, NX - 1) if r < 2 else (NX - 1, 1)

    def y_copy(r, idx, pos, dev):
        ref = y_ref(r, *pos)
        return rcopy(ref, ref, y_send.at[r, idx], y_recv.at[r, idx], dev)

    def y_second(r, j, a):
        d2 = y_dir(r)[1]
        pos = y_pos(r, a, 0)
        go(y_copy(r, 3 + 3 * j, pos, tpdev(*y_pos(r, 0, d2))))
        go(y_copy(r, 4 + 3 * j, pos, tpdev(*y_pos(r, 0, NX - d2))))

    def y_start(r):
        d = y_dir(r)[0]
        pos = y_pos(r, 0, 0)
        go(y_copy(r, 0, pos, tpdev(*y_pos(r, d, 0))))
        go(y_copy(r, 1, pos, tpdev(*y_pos(r, NX - d, 0))))
        y_second(r, 0, 0)

    def y_mid(r):
        d = y_dir(r)[0]
        y_copy(r, 0, y_pos(r, NX - d, 0), partner).wait_recv()
        go(y_copy(r, 2, y_pos(r, NX - d, 0), tpdev(*y_pos(r, d, 0))))
        y_second(r, 1, NX - d)
        y_copy(r, 1, y_pos(r, d, 0), partner).wait_recv()
        y_second(r, 2, d)
        y_copy(r, 2, y_pos(r, 2, 0), partner).wait_recv()
        y_second(r, 3, 2)

    def y_offs(r):
        d = y_dir(r)[0]
        return (0, NX - d, d, 2)

    def y_fwd(r):
        d2 = y_dir(r)[1]
        for j, a in enumerate(y_offs(r)):
            pos = y_pos(r, a, NX - d2)
            y_copy(r, 3 + 3 * j, pos, partner).wait_recv()
            go(y_copy(r, 5 + 3 * j, pos, tpdev(*y_pos(r, 0, d2))))

    def y_end(r):
        d2 = y_dir(r)[1]
        for j, a in enumerate(y_offs(r)):
            y_copy(r, 4 + 3 * j, y_pos(r, a, d2), partner).wait_recv()
            y_copy(r, 5 + 3 * j, y_pos(r, a, 2), partner).wait_recv()
        out = pltpu.make_async_copy(yg.at[pl.ds(r * RL, RL), :], y_hbm.at[pl.ds(r * RL, RL), :], out_sem.at[r])
        out.start()
        return out

    def matmul(r, half):
        out = psend if half == 0 else pown
        hh = (1 - yh) if half == 0 else yh
        for n in range(2):
            cols = pl.ds(pl.multiple_of(hh * F + n * 256, 256), 256)
            out[r, :, n * 256:(n + 1) * 256] = jnp.dot(og[r * RL:(r + 1) * RL, :], wt[:, cols], preferred_element_type=F32)

    rs_dev = tpdev(z, 3 - y)

    def rs_copy(r):
        return rcopy(psend.at[r], rsb.at[r], r_send.at[r], r_recv.at[r], rs_dev)

    def rs_finish(r):
        rs_copy(r).wait_recv()
        yg[r * RL:(r + 1) * RL, pl.ds(pl.multiple_of(piece_of(z, y) * F, F), F)] = (pown[r] + rsb[r]).astype(BF)

    for r in range(R):
        o_copy(r, 0, z, 1, partner).wait_recv()
        o_send_z(r, 1)
        o_mid_z(r, 0)
    wo_own.wait()
    for dz, e in group:
        w_fwd(dz, e, 1 - k).wait_recv()
    for r in range(R):
        o_mid_z(r, 1)
        o_end_z(r, 0)
        o_end_z(r, 1)
        matmul(r, 0)
        go(rs_copy(r))
        matmul(r, 1)
        if r >= 1:
            rs_finish(r - 1)
            y_start(r - 1)
        if r >= 2:
            y_mid(r - 2)
    rs_finish(R - 1)
    y_start(R - 1)
    y_mid(R - 2)
    y_mid(R - 1)
    for r in range(R):
        y_fwd(r)
    outs = [y_end(r) for r in range(R)]

    for cp_ in sends:
        cp_.wait_send()

    @pl.when(xodd == 1)
    def _():
        q_d2d.wait_send()

    for xx in range(NX):
        @pl.when(jnp.logical_not((x == xx) & (xodd == 0)))
        def _():
            rcopy(obuf.at[xx], obuf.at[xx], o_send.at[xx], o_recv.at[x], partner).wait_send()
    for out in outs:
        out.wait()


def solution(mesh):
    def body(x, doc, wq, wk, wv, wo):
        seg = jnp.broadcast_to(doc[None, :], (8, L))
        dma = pltpu.SemaphoreType.DMA
        any_ = pl.BlockSpec(memory_space=pl.ANY)
        return pl.pallas_call(
            kernel,
            out_shape=jax.ShapeDtypeStruct((L, D), BF),
            in_specs=[any_] * 6,
            out_specs=any_,
            scratch_shapes=[
                pltpu.VMEM((NKC, L, KC), BF), pltpu.VMEM((NB, KC, F), BF), pltpu.VMEM((L, F), F32),
                pltpu.VMEM((4, L, HD), BF), pltpu.VMEM((4, L, HD), BF), pltpu.VMEM((4, L, HD), BF),
                pltpu.VMEM((8, L, HD), BF), pltpu.VMEM((8, L, HD), BF), pltpu.VMEM((4, L, HD), BF), pltpu.VMEM((4, L, HD), BF),
                pltpu.VMEM((L, 8 * F), BF), pltpu.VMEM((8 * F, 1024), BF),
                pltpu.VMEM((R, RL, F), F32), pltpu.VMEM((R, RL, F), F32), pltpu.VMEM((R, RL, F), F32),
                pltpu.VMEM((L, D), BF), pltpu.VMEM((8, 8, L), jnp.int32), pltpu.VMEM((L, HD), jnp.int32),
                pltpu.VMEM((L, HD), F32), pltpu.VMEM((L, HD), F32), pltpu.VMEM((L, HD), F32),
                dma((NKC,)), dma((NB,)), dma, dma((7,)), dma((7,)), dma((7,)), dma((7,)),
                dma((2, 4)), dma((2, 4)), dma((2, 3)), dma((2, 3)), dma((4,)), dma((4,)), dma((4,)), dma((4,)),
                dma((7,)), dma((7,)), dma, dma((R, 7)), dma((R, 7)), dma((R,)), dma((R,)), dma((R, 15)), dma((R, 15)), dma((R,)),
            ],
            compiler_params=pltpu.CompilerParams(collective_id=0, has_side_effects=True, vmem_limit_bytes=60 * 1024 * 1024),
        )(x, seg, wq, wk, wv, wo)

    return jax.shard_map(body, mesh=mesh, in_specs=(P(('dp', 'cp'), None), P(('dp', 'cp')), P(None, 'tp'), P(None, 'tp'), P(None, 'tp'), P('tp', None)), out_specs=P(('dp', 'cp'), None), check_vma=False)
```

```python
import jax
import jax.numpy as jnp
from jax import lax
from jax.experimental import pallas as pl
from jax.experimental.pallas import tpu as pltpu
from jax.sharding import PartitionSpec as P

MESH = pl.DeviceIdType.MESH
HD = 128
NX = 4
L = 512
D = 8192
F = 512
KC = 1024
NKC = D // KC
NB = 6
ROWS = ((0, 64), (64, 64), (128, 128), (256, 128), (384, 64), (448, 64))
R = len(ROWS)
Y_ORDER = (0, 0, 1, 0, 1, 1)
Y_DIR = ((1, 3), (1, 3), (3, 1), (1, 1), (1, 3), (1, 3))
O_DIR = (1, 1, 3, 3, 1, 3)
ORDER = (
    ("ostart", 1), ("ostart", 5), ("ostart", 0), ("opair", 1), ("opair", 5), ("opair", 0),
    ("ofw0", 5), ("ofw1", 1), ("ofw1", 5), ("ofw0", 1), ("ofw0", 0), ("ostart", 2),
    ("ofw1", 0), ("mm0", 1), ("mm0", 5), ("opair", 2), ("ofw0", 2), ("mm1", 1),
    ("mm0", 0), ("ofw1", 2), ("ostart", 4), ("mm1", 0), ("mm1", 5), ("yst", 1),
    ("yst", 5), ("yst", 0), ("ofw0", 4), ("opair", 4), ("mm0", 2), ("mm1", 2),
    ("ostart", 3), ("ofw1", 4), ("opair", 3), ("ym0", 0), ("ym0", 1), ("ym1", 1),
    ("ofw0", 3), ("mm0", 4), ("mm1", 4), ("ofw1", 3), ("yst", 2), ("ym2", 1),
    ("ym1", 5), ("yst", 4), ("mm0", 3), ("ym0", 2), ("ym1", 0), ("ym0", 4),
    ("mm1", 3), ("ym2", 0), ("yf", 2, 0), ("yf", 1, 0), ("ym1", 4), ("yst", 3),
    ("ym0", 5), ("ym2", 4), ("yf", 0, 3), ("yf", 0, 2), ("yf", 5, 0), ("ym0", 3),
    ("yf", 0, 0), ("yf", 4, 3), ("ym2", 5), ("yf", 5, 1), ("ym2", 2), ("yf", 1, 2),
    ("yf", 4, 1), ("yf", 1, 3), ("yf", 4, 2), ("ym1", 3), ("ym1", 2), ("yf", 0, 1),
    ("yf", 3, 1), ("yf", 3, 0), ("yf", 1, 1), ("ym2", 3), ("yf", 2, 3), ("yf", 3, 2),
    ("yf", 2, 1), ("yf", 4, 0), ("yf", 5, 2), ("yf", 2, 2), ("yf", 5, 3), ("yf", 3, 3),
    ("ye", 2), ("ye", 0), ("ye", 5), ("ye", 4), ("ye", 1), ("ye", 3),
)
QT = 256
SCALE = (HD ** -0.5) * 1.4426950408889634
BF = jnp.bfloat16
F32 = jnp.float32


def mod(a, n):
    return lax.rem(a + n, n)


def kernel(x_hbm, seg_hbm, wq_hbm, wk_hbm, wv_hbm, wo_hbm, yg,
           xbuf, wbuf, acc, kloc, vloc, qloc, kg, vg, qg, obuf, og, wt, psend, pown, rsb, segs, sq, m_s, l_s, o_s,
           x_sem, w_sem, wo_sem, ws_send, ws_recv, wf_send, wf_recv,
           kv_send, kv_recv, kf_send, kf_recv, q_send, q_recv, o_send, o_recv,
           sg_send, sg_recv, sg_loc, a_send, a_recv, r_send, r_recv, y_send, y_recv):
    t = lax.axis_index("tp")
    c = lax.axis_index("cp")
    x, k = c // 2, lax.rem(c, 2)
    z, y = t // NX, lax.rem(t, NX)
    yh, yb = y // 2, lax.rem(y, 2)
    xodd = lax.rem(x, 2)
    partner = {"cp": x * 2 + 1 - k}

    def iy(yy):
        return lax.rem(yy + yy // 2, 2)

    def slice_of(zz, yy):
        return zz * 2 + iy(yy)

    def piece_of(zz, yy):
        return slice_of(zz, yy) * 2 + yy // 2

    def tpdev(zz, yy):
        return {"tp": zz * NX + yy}

    def rcopy(src, dst, ss, rs, dev):
        return pltpu.make_async_remote_copy(src_ref=src, dst_ref=dst, send_sem=ss, recv_sem=rs, device_id=dev, device_id_type=MESH)

    s_me = z * 2 + yb
    sl_me = slice_of(z, y)
    sends = []

    def x_copy(i):
        return pltpu.make_async_copy(x_hbm.at[:, pl.ds(pl.multiple_of(i * KC, KC), KC)], xbuf.at[i], x_sem.at[i])

    w_hbms = (wk_hbm, wv_hbm, wq_hbm)

    def w_copies(w, i):
        g = lax.rem(4 * w + i, 3) * 2
        return [pltpu.make_async_copy(w_hbms[w].at[pl.ds(pl.multiple_of((2 * i + b) * KC, KC), KC), :], wbuf.at[g + b], w_sem.at[g + b]) for b in range(2)]

    def load(w, i):
        for b, cp_ in enumerate(w_copies(w, i)):
            if w == 0:
                x_copy(2 * i + b).start()
            cp_.start()

    for i in range(2):
        load(0, jnp.int32(i))
    seg_own = pltpu.make_async_copy(seg_hbm, segs.at[c], sg_loc)
    seg_own.start()
    wo_own = pltpu.make_async_copy(wo_hbm.at[:, pl.ds(pl.multiple_of(sl_me * 1024, 1024), 1024)],
                                   wt.at[pl.ds(pl.multiple_of(s_me * F, F), F), :], wo_sem)

    bar = pltpu.get_barrier_semaphore()
    n_peers = 0
    for dc in range(1, 2 * NX):
        pl.semaphore_signal(bar, inc=1, device_id={"cp": mod(c + dc, 2 * NX)}, device_id_type=MESH)
        n_peers += 1
    for dz in range(NX):
        for e in range(2):
            if dz or e:
                pl.semaphore_signal(bar, inc=1, device_id=tpdev(mod(z + dz, NX), yh * 2 + lax.rem(yb + e, 2)), device_id_type=MESH)
                n_peers += 1
    pl.semaphore_signal(bar, inc=1, device_id=tpdev(z, 3 - y), device_id_type=MESH)
    n_peers += 1

    def w_move(dz, e):
        z2, y2 = mod(z + dz, NX), yh * 2 + lax.rem(yb + e, 2)
        i = dz * 2 + e - 1
        return rcopy(wo_hbm.at[pl.ds(pl.multiple_of(k * 256, 256), 256), pl.ds(pl.multiple_of(slice_of(z2, y2) * 1024, 1024), 1024)],
                     wt.at[pl.ds(pl.multiple_of(s_me * F + k * 256, 256), 256), :],
                     ws_send.at[i], ws_recv.at[i], tpdev(z2, y2))

    def w_rows(dz, e, kk):
        s = mod(z - dz, NX) * 2 + lax.rem(yb + e, 2)
        return wt.at[pl.ds(pl.multiple_of(s * F + kk * 256, 256), 256), :]

    def w_fwd(dz, e, kk):
        i = dz * 2 + e - 1
        ref = w_rows(dz, e, kk)
        return rcopy(ref, ref, wf_send.at[i], wf_recv.at[i], partner)

    group = [(dz, e) for dz in range(NX) for e in range(2) if dz or e]
    def spread_w():
        pl.semaphore_wait(bar, n_peers)
        seg_own.wait()
        for dc in range(1, 2 * NX):
            cp_ = rcopy(segs.at[c], segs.at[c], sg_send.at[dc - 1], sg_recv.at[dc - 1], {"cp": mod(c + dc, 2 * NX)})
            cp_.start()
            sends.append(cp_)
        for dz, e in group:
            cp_ = w_move(dz, e)
            cp_.start()
            sends.append(cp_)
        wo_own.start()

    def project(w, lo, hi):
        def step(i, _):
            nxt = i + 2

            @pl.when(nxt < NKC // 2)
            def _():
                load(w, nxt)
            if w < 2:
                @pl.when(nxt >= NKC // 2)
                def _():
                    load(w + 1, nxt - NKC // 2)
            for b, cp_ in enumerate(w_copies(w, i)):
                cp_.wait()
                if w == 0:
                    x_copy(2 * i + b).wait()
            g = lax.rem(4 * w + i, 3) * 2
            acc[...] += (jnp.dot(xbuf[2 * i], wbuf[g], preferred_element_type=F32)
                         + jnp.dot(xbuf[2 * i + 1], wbuf[g + 1], preferred_element_type=F32))
            return 0
        lax.fori_loop(lo, hi, step, 0)

    def split(dst):
        for h in range(4):
            dst[h] = acc[:, h * HD:(h + 1) * HD].astype(BF)

    def kv_spread(n, loc, gat):
        for dx in range(1, NX):
            h = mod(x + dx, NX)
            cp_ = rcopy(loc.at[h], gat.at[c], kv_send.at[n, dx - 1], kv_recv.at[n, dx - 1], {"cp": h * 2 + k})
            cp_.start()
            sends.append(cp_)
        cp_ = rcopy(loc.at[x], gat.at[c], kv_send.at[n, 3], kv_recv.at[n, 3], partner)
        cp_.start()
        sends.append(cp_)
        gat[c] = loc[x]

    def kv_forward(n, gat):
        for dx in (1, 3, 2):
            ref = gat.at[mod(x - dx, NX) * 2 + k]
            rcopy(ref, ref, kv_send.at[n, dx - 1], kv_recv.at[n, dx - 1], partner).wait_recv()
            cp_ = rcopy(ref, ref, kf_send.at[n, dx - 1], kf_recv.at[n, dx - 1], partner)
            cp_.start()
            sends.append(cp_)

    def kv_finish(n, gat):
        ref = gat.at[x * 2 + 1 - k]
        rcopy(ref, ref, kv_send.at[n, 3], kv_recv.at[n, 3], partner).wait_recv()
        for dx in (1, 3, 2):
            ref = gat.at[mod(x - dx, NX) * 2 + 1 - k]
            rcopy(ref, ref, kf_send.at[n, dx - 1], kf_recv.at[n, dx - 1], partner).wait_recv()

    acc[...] = jnp.zeros_like(acc)
    with jax.named_scope("proj_k0"):
        project(0, 0, 2)
    with jax.named_scope("barrier"):
        spread_w()
    with jax.named_scope("proj_k1"):
        project(0, 2, 4)
    split(kloc)
    acc[...] = jnp.zeros_like(acc)
    kv_spread(0, kloc, kg)
    with jax.named_scope("proj_v"):
        project(1, 0, 4)
    split(vloc)
    acc[...] = jnp.zeros_like(acc)
    kv_spread(1, vloc, vg)
    with jax.named_scope("proj_q0"):
        project(2, 0, 2)
    with jax.named_scope("fwd_k"):
        kv_forward(0, kg)
    with jax.named_scope("proj_q1"):
        project(2, 2, 4)
    split(qloc)
    own = lax.rem(x + k, 2)
    for dx in (2, 1, 3):
        h = mod(x + dx, NX)
        cp_ = rcopy(qloc.at[h], qg.at[x], q_send.at[dx - 1], q_recv.at[x], {"cp": h * 2 + own})
        cp_.start()
        sends.append(cp_)

    @pl.when(xodd == 0)
    def _():
        qg[x] = qloc[x]

    q_d2d = rcopy(qloc.at[x], qg.at[x], q_send.at[3], q_recv.at[x], partner)

    @pl.when(xodd == 1)
    def _():
        q_d2d.start()

    with jax.named_scope("fwd_v"):
        kv_forward(1, vg)

    with jax.named_scope("fin_kv"):
        kv_finish(0, kg)
        kv_finish(1, vg)
    for dc in range(1, 2 * NX):
        ref = segs.at[mod(c - dc, 2 * NX)]
        rcopy(ref, ref, sg_send.at[dc - 1], sg_recv.at[dc - 1], partner).wait_recv()

    for xx in range(NX):
        c_q = 2 * xx + lax.rem(k + xx, 2)
        local = (x == xx) & (xodd == 0)

        @pl.when(jnp.logical_not(local))
        def _():
            rcopy(qg.at[xx], qg.at[xx], q_send.at[3], q_recv.at[xx], partner).wait_recv()

        sq[...] = jnp.transpose(jnp.broadcast_to(segs[c_q], (HD, L)))

        def block(j, rows, diag):
            s = lax.dot_general(qg[xx, rows, :], kg[j], (((1,), (1,)), ((), ())), preferred_element_type=F32)
            ok = jnp.concatenate([sq[rows, :]] * (L // HD), axis=1) == jnp.broadcast_to(segs[j], (QT, L))
            if diag:
                ri = lax.broadcasted_iota(jnp.int32, (QT, L), 0) + rows.start
                ok = ok & (ri >= lax.broadcasted_iota(jnp.int32, (QT, L), 1))
            return jnp.where(ok, s * SCALE, -jnp.inf)

        tiles = [slice(a, a + QT) for a in range(0, L, QT)]
        with jax.named_scope("attn%d" % xx):
            for rows in tiles:
                s = block(c_q, rows, True)
                m0 = jnp.broadcast_to(jnp.max(s, axis=1, keepdims=True), (QT, HD))
                p = jnp.exp2(s - jnp.concatenate([m0] * (L // HD), axis=1))
                m_s[rows, :] = m0
                l_s[rows, :] = jnp.broadcast_to(jnp.sum(p, axis=1, keepdims=True), (QT, HD))
                o_s[rows, :] = jnp.dot(p.astype(BF), vg[c_q], preferred_element_type=F32)

            def kv_step(j, _):
                for rows in tiles:
                    s = block(j, rows, False)
                    m_old = m_s[rows, :]
                    m_new = jnp.maximum(m_old, jnp.max(s, axis=1, keepdims=True))
                    alpha = jnp.exp2(m_old - m_new)
                    p = jnp.exp2(s - jnp.concatenate([m_new] * (L // HD), axis=1))
                    m_s[rows, :] = m_new
                    l_s[rows, :] = l_s[rows, :] * alpha + jnp.sum(p, axis=1, keepdims=True)
                    o_s[rows, :] = o_s[rows, :] * alpha + jnp.dot(p.astype(BF), vg[j], preferred_element_type=F32)
                return 0
            lax.fori_loop(0, c_q, kv_step, 0)
            for rows in tiles:
                obuf[xx, rows, :] = (o_s[rows, :] / l_s[rows, :]).astype(BF)

        ocol = pl.ds(pl.multiple_of(s_me * F + x * HD, HD), HD)
        o_ret = rcopy(obuf.at[xx], og.at[:, ocol], o_send.at[xx], o_recv.at[x], {"cp": c_q})

        @pl.when(local)
        def _():
            og[:, ocol] = obuf[xx]

        @pl.when(jnp.logical_not(local))
        def _():
            o_ret.start()

    for h in range(NX):
        ref = og.at[:, pl.ds(pl.multiple_of(s_me * F + h * HD, HD), HD)]

        @pl.when(jnp.logical_not((x == h) & (xodd == 0)))
        def _():
            rcopy(obuf.at[0], ref, o_send.at[0], o_recv.at[h], partner).wait_recv()

    def go(cp_):
        cp_.start()
        sends.append(cp_)

    def row_ds(r):
        return pl.ds(ROWS[r][0], ROWS[r][1])

    def o_copy(r, idx, zz, e, dev):
        s = zz * 2 + lax.rem(yb + e, 2)
        ref = og.at[row_ds(r), pl.ds(pl.multiple_of(s * F, F), F)]
        return rcopy(ref, ref, a_send.at[r, idx], a_recv.at[r, idx], dev)

    def o_send_z(r, e):
        d = O_DIR[r]
        go(o_copy(r, 1 + 3 * e, z, e, tpdev(mod(z + d, NX), y)))
        go(o_copy(r, 2 + 3 * e, z, e, tpdev(mod(z + NX - d, NX), y)))

    def o_forward(r, e):
        d = O_DIR[r]
        zz = mod(z + NX - d, NX)
        o_copy(r, 1 + 3 * e, zz, e, partner).wait_recv()
        go(o_copy(r, 3 + 3 * e, zz, e, tpdev(mod(z + d, NX), y)))

    def ostart(r):
        go(o_copy(r, 0, z, 0, tpdev(z, yh * 2 + 1 - yb)))
        o_send_z(r, 0)

    def opair(r):
        o_copy(r, 0, z, 1, partner).wait_recv()
        o_send_z(r, 1)

    def o_rest(r):
        for e in range(2):
            o_copy(r, 2 + 3 * e, mod(z + O_DIR[r], NX), e, partner).wait_recv()
            o_copy(r, 3 + 3 * e, mod(z + 2, NX), e, partner).wait_recv()

    def matmul(r, half):
        out = psend if half == 0 else pown
        hh = (1 - yh) if half == 0 else yh
        a, n = ROWS[r]
        for b in range(2):
            cols = pl.ds(pl.multiple_of(hh * F + b * 256, 256), 256)
            out[a:a + n, b * 256:(b + 1) * 256] = jnp.dot(og[a:a + n, :], wt[:, cols], preferred_element_type=F32)

    def rs_copy(r):
        return rcopy(psend.at[row_ds(r), :], rsb.at[row_ds(r), :], r_send.at[r], r_recv.at[r], tpdev(z, 3 - y))

    def mm0(r):
        o_rest(r)
        if r == first_mm:
            wo_own.wait()
            for dz, e in group:
                w_fwd(dz, e, 1 - k).wait_recv()
        matmul(r, 0)
        go(rs_copy(r))

    def y_pos(r, a, b):
        if Y_ORDER[r] == 0:
            return mod(z + a, NX), mod(y + b, NX)
        return mod(z + b, NX), mod(y + a, NX)

    def y_ref(r, pos):
        return yg.at[row_ds(r), pl.ds(pl.multiple_of(piece_of(*pos) * F, F), F)]

    def y_copy(r, idx, pos, dev):
        ref = y_ref(r, pos)
        return rcopy(ref, ref, y_send.at[r, idx], y_recv.at[r, idx], dev)

    def y_second(r, j, a):
        d2 = Y_DIR[r][1]
        pos = y_pos(r, a, 0)
        go(y_copy(r, 3 + 3 * j, pos, tpdev(*y_pos(r, 0, d2))))
        go(y_copy(r, 4 + 3 * j, pos, tpdev(*y_pos(r, 0, NX - d2))))

    def yst(r):
        rs_copy(r).wait_recv()
        a, n = ROWS[r]
        yg[a:a + n, pl.ds(pl.multiple_of(piece_of(z, y) * F, F), F)] = (pown[a:a + n, :] + rsb[a:a + n, :]).astype(BF)
        d = Y_DIR[r][0]
        pos = y_pos(r, 0, 0)
        go(y_copy(r, 0, pos, tpdev(*y_pos(r, d, 0))))
        go(y_copy(r, 1, pos, tpdev(*y_pos(r, NX - d, 0))))
        y_second(r, 0, 0)

    def ym0(r):
        d = Y_DIR[r][0]
        pos = y_pos(r, NX - d, 0)
        y_copy(r, 0, pos, partner).wait_recv()
        go(y_copy(r, 2, pos, tpdev(*y_pos(r, d, 0))))
        y_second(r, 1, NX - d)

    def ym1(r):
        d = Y_DIR[r][0]
        y_copy(r, 1, y_pos(r, d, 0), partner).wait_recv()
        y_second(r, 2, d)

    def ym2(r):
        y_copy(r, 2, y_pos(r, 2, 0), partner).wait_recv()
        y_second(r, 3, 2)

    def y_offs(r):
        d = Y_DIR[r][0]
        return (0, NX - d, d, 2)

    def yf(r, j):
        d2 = Y_DIR[r][1]
        pos = y_pos(r, y_offs(r)[j], NX - d2)
        y_copy(r, 3 + 3 * j, pos, partner).wait_recv()
        go(y_copy(r, 5 + 3 * j, pos, tpdev(*y_pos(r, 0, d2))))

    def ye(r):
        d2 = Y_DIR[r][1]
        for j, a in enumerate(y_offs(r)):
            y_copy(r, 4 + 3 * j, y_pos(r, a, d2), partner).wait_recv()
            y_copy(r, 5 + 3 * j, y_pos(r, a, 2), partner).wait_recv()

    steps = dict(ostart=ostart, opair=opair, ofw0=lambda r: o_forward(r, 0), ofw1=lambda r: o_forward(r, 1), mm0=mm0,
                 mm1=lambda r: matmul(r, 1), yst=yst, ym0=ym0, ym1=ym1, ym2=ym2, yf=yf, ye=ye)
    first_mm = [a[1] for a in ORDER if a[0] == "mm0"][0]
    started = False
    for name, *args in ORDER:
        if not started and name != "ostart":
            started = True
            for dz, e in group:
                i = dz * 2 + e - 1
                with jax.named_scope("wait_w%d" % i):
                    ref = w_rows(dz, e, k)
                    rcopy(ref, ref, ws_send.at[i], ws_recv.at[i], partner).wait_recv()
                    go(w_fwd(dz, e, k))
        with jax.named_scope(name + "_".join(str(a) for a in args)):
            steps[name](*args)

    for cp_ in sends:
        cp_.wait_send()

    @pl.when(xodd == 1)
    def _():
        q_d2d.wait_send()

    for xx in range(NX):
        @pl.when(jnp.logical_not((x == xx) & (xodd == 0)))
        def _():
            rcopy(obuf.at[xx], obuf.at[xx], o_send.at[xx], o_recv.at[x], partner).wait_send()


def solution(mesh):
    def body(x, doc, wq, wk, wv, wo):
        seg = doc.reshape(1, L)
        dma = pltpu.SemaphoreType.DMA
        any_ = pl.BlockSpec(memory_space=pl.ANY)
        return pl.pallas_call(
            kernel,
            out_shape=pltpu.VMEM((L, D), BF),
            in_specs=[any_] * 6,
            out_specs=pl.BlockSpec(memory_space=pltpu.VMEM),
            scratch_shapes=[
                pltpu.VMEM((NKC, L, KC), BF), pltpu.VMEM((NB, KC, F), BF), pltpu.VMEM((L, F), F32),
                pltpu.VMEM((4, L, HD), BF), pltpu.VMEM((4, L, HD), BF), pltpu.VMEM((4, L, HD), BF),
                pltpu.VMEM((8, L, HD), BF), pltpu.VMEM((8, L, HD), BF), pltpu.VMEM((4, L, HD), BF), pltpu.VMEM((4, L, HD), BF),
                pltpu.VMEM((L, 8 * F), BF), pltpu.VMEM((8 * F, 1024), BF),
                pltpu.VMEM((L, F), F32), pltpu.VMEM((L, F), F32), pltpu.VMEM((L, F), F32),
                pltpu.VMEM((8, 1, L), jnp.int32), pltpu.VMEM((L, HD), jnp.int32),
                pltpu.VMEM((L, HD), F32), pltpu.VMEM((L, HD), F32), pltpu.VMEM((L, HD), F32),
                dma((NKC,)), dma((NB,)), dma, dma((7,)), dma((7,)), dma((7,)), dma((7,)),
                dma((2, 4)), dma((2, 4)), dma((2, 3)), dma((2, 3)), dma((4,)), dma((4,)), dma((4,)), dma((4,)),
                dma((7,)), dma((7,)), dma, dma((R, 7)), dma((R, 7)), dma((R,)), dma((R,)), dma((R, 15)), dma((R, 15)),
            ],
            compiler_params=pltpu.CompilerParams(collective_id=0, has_side_effects=True, vmem_limit_bytes=50 * 1024 * 1024),
        )(x, seg, wq, wk, wv, wo)

    return jax.shard_map(body, mesh=mesh, in_specs=(P(('dp', 'cp'), None), P(('dp', 'cp')), P(None, 'tp'), P(None, 'tp'), P(None, 'tp'), P('tp', None)), out_specs=P(('dp', 'cp'), None), check_vma=False)
```

```python
import jax
import jax.numpy as jnp
from jax import lax
from jax.experimental import pallas as pl
from jax.experimental.pallas import tpu as pltpu
from jax.sharding import PartitionSpec as P

MESH = pl.DeviceIdType.MESH
HD = 128
NX = 4
L = 512
D = 8192
F = 512
KC = 1024
NKC = D // KC
NB = 6
ROWS = ((0, 64), (64, 64), (128, 64), (192, 64), (256, 64), (320, 64), (384, 64), (448, 64))
R = len(ROWS)
Y_ORDER = (1, 1, 0, 1, 1, 0, 1, 0)
Y_DIR = ((3, 1), (3, 1), (3, 1), (1, 3), (3, 3), (3, 3), (3, 1), (3, 1))
O_FIRST = (0, 1, 0, 1, 0, 1, 0, 0)
O_DIR = (1, 1, 3, 3, 3, 1, 3, 3)
ORDER = (
    ("ostart", 3,), ("ostart", 0,), ("ostart", 2,), ("opair", 3,), ("ostart", 1,), ("ofw0", 0,),
    ("ofw0", 3,), ("opair", 0,), ("opair", 2,), ("ofw1", 3,), ("opair", 1,), ("wxl",),
    ("ostart", 5,), ("ofw1", 0,), ("ostart", 7,), ("ofw0", 2,), ("ofw0", 1,), ("mm0", 3,),
    ("mm1", 3,), ("opair", 5,), ("mm0", 0,), ("ofw1", 1,), ("opair", 7,), ("ostart", 6,),
    ("ofw0", 7,), ("ofw1", 2,), ("yst", 3,), ("ofw0", 5,), ("ofw1", 5,), ("mm0", 1,),
    ("mm1", 0,), ("ostart", 4,), ("yst", 0,), ("ofw1", 7,), ("ofw0", 6,), ("mm0", 2,),
    ("ym1", 3,), ("ym0", 3,), ("mm0", 5,), ("mm1", 2,), ("ofw0", 4,), ("ym0", 0,),
    ("mm1", 1,), ("yst", 2,), ("mm0", 7,), ("opair", 4,), ("yst", 1,), ("ym1", 0,),
    ("ym2", 3,), ("mm1", 5,), ("ofw1", 4,), ("ym2", 0,), ("yf", 0, 0,), ("opair", 6,),
    ("ofw1", 6,), ("yst", 5,), ("mm1", 7,), ("yst", 7,), ("yf", 0, 3,), ("yf", 0, 1,),
    ("yf", 3, 0,), ("mm0", 4,), ("mm0", 6,), ("ym1", 1,), ("ym0", 1,), ("mm1", 6,),
    ("ym0", 2,), ("yf", 2, 0,), ("mm1", 4,), ("yf", 3, 3,), ("yf", 0, 2,), ("yst", 4,),
    ("yf", 1, 1,), ("yst", 6,), ("yf", 2, 1,), ("ym2", 1,), ("yf", 1, 2,), ("ym0", 7,),
    ("ym0", 5,), ("ym1", 5,), ("yf", 3, 2,), ("ym0", 4,), ("yf", 6, 0,), ("ym1", 2,),
    ("ym1", 4,), ("yf", 5, 1,), ("yf", 4, 0,), ("yf", 7, 0,), ("yf", 1, 3,), ("ym1", 7,),
    ("ym2", 7,), ("ym0", 6,), ("yf", 5, 0,), ("yf", 2, 2,), ("yf", 3, 1,), ("yf", 1, 0,),
    ("ym2", 2,), ("ym2", 4,), ("yf", 4, 1,), ("yf", 7, 3,), ("ye", 0,), ("yf", 7, 1,),
    ("ym1", 6,), ("yf", 4, 2,), ("ym2", 5,), ("ym2", 6,), ("yf", 6, 1,), ("yf", 2, 3,),
    ("yf", 5, 2,), ("yf", 7, 2,), ("yf", 4, 3,), ("yf", 6, 2,), ("ye", 1,), ("yf", 5, 3,),
    ("yf", 6, 3,), ("ye", 3,), ("ye", 5,), ("ye", 7,), ("ye", 2,), ("ye", 4,),
    ("ye", 6,),
)
HL = L // 2
SCALE = (HD ** -0.5) * 1.4426950408889634
U = 16
DR = L - 8 * U
BF = jnp.bfloat16
F32 = jnp.float32


def mod(a, n):
    return lax.rem(a + n, n)


def kernel(x_hbm, seg_hbm, wq_hbm, wk_hbm, wv_hbm, wo_hbm, yg,
           xbuf, wbuf, acc, kloc, vloc, qloc, kg, vg, qg, obuf, og, wt, psend, pown, rsb, segs, sk, m_s, l_s, o_s,
           x_sem, w_sem, wo_sem, ws_send, ws_recv, wf_send, wf_recv, sh_send, sh_recv, wx_send, wx_recv,
           kv_send, kv_recv, kf_send, kf_recv, q_send, q_recv, o_send, o_recv,
           sg_send, sg_recv, sg_loc, a_send, a_recv, r_send, r_recv, y_send, y_recv):
    t = lax.axis_index("tp")
    c = lax.axis_index("cp")
    x, k = c // 2, lax.rem(c, 2)
    z, y = t // NX, lax.rem(t, NX)
    yh, yb = y // 2, lax.rem(y, 2)
    xodd = lax.rem(x, 2)
    partner = {"cp": x * 2 + 1 - k}

    def iy(yy):
        return lax.rem(yy + yy // 2, 2)

    def slice_of(zz, yy):
        return zz * 2 + iy(yy)

    def piece_of(zz, yy):
        return slice_of(zz, yy) * 2 + yy // 2

    def tpdev(zz, yy):
        return {"tp": zz * NX + yy}

    def rcopy(src, dst, ss, rs, dev):
        return pltpu.make_async_remote_copy(src_ref=src, dst_ref=dst, send_sem=ss, recv_sem=rs, device_id=dev, device_id_type=MESH)

    s_me = z * 2 + yb
    sl_me = slice_of(z, y)
    sends = []

    def x_copy(i):
        return pltpu.make_async_copy(x_hbm.at[:, pl.ds(pl.multiple_of(i * KC, KC), KC)], xbuf.at[i], x_sem.at[i])

    w_hbms = (wk_hbm, wv_hbm, wq_hbm)

    def w_copies(w, i):
        g = lax.rem(4 * w + i, 3) * 2
        return [pltpu.make_async_copy(w_hbms[w].at[pl.ds(pl.multiple_of((2 * i + b) * KC, KC), KC), :], wbuf.at[g + b], w_sem.at[g + b]) for b in range(2)]

    def load(w, i):
        for b, cp_ in enumerate(w_copies(w, i)):
            if w == 0:
                x_copy(2 * i + b).start()
            cp_.start()

    for i in range(2):
        load(0, jnp.int32(i))
    seg_own = pltpu.make_async_copy(seg_hbm, segs.at[c], sg_loc)
    seg_own.start()
    my_cols = pl.ds(pl.multiple_of(sl_me * 1024, 1024), 1024)

    def share(cc):
        return pl.ds(pl.multiple_of(DR + cc * U, U), U)

    wo_own = [pltpu.make_async_copy(wo_hbm.at[pl.ds(0, DR), my_cols], wt.at[s_me, pl.ds(0, DR), :], wo_sem.at[0]),
              pltpu.make_async_copy(wo_hbm.at[share(c), my_cols], wt.at[s_me, share(c), :], wo_sem.at[1])]

    bar = pltpu.get_barrier_semaphore()
    n_peers = 0
    for dc in range(1, 2 * NX):
        pl.semaphore_signal(bar, inc=1, device_id={"cp": mod(c + dc, 2 * NX)}, device_id_type=MESH)
        n_peers += 1
    for dz in range(NX):
        for e in range(2):
            if dz or e:
                pl.semaphore_signal(bar, inc=1, device_id=tpdev(mod(z + dz, NX), yh * 2 + lax.rem(yb + e, 2)), device_id_type=MESH)
                n_peers += 1
    pl.semaphore_signal(bar, inc=1, device_id=tpdev(z, 3 - y), device_id_type=MESH)
    n_peers += 1

    HR = DR // 2

    def w_move(dz, e, shared):
        z2, y2 = mod(z + dz, NX), yh * 2 + lax.rem(yb + e, 2)
        i = dz * 2 + e - 1
        rows = share(c) if shared else pl.ds(pl.multiple_of(k * HR, HR), HR)
        return rcopy(wo_hbm.at[rows, pl.ds(pl.multiple_of(slice_of(z2, y2) * 1024, 1024), 1024)], wt.at[s_me, rows, :],
                     sh_send.at[i] if shared else ws_send.at[i], sh_recv.at[i] if shared else ws_recv.at[i], tpdev(z2, y2))

    def w_slot(dz, e):
        return mod(z - dz, NX) * 2 + lax.rem(yb + e, 2)

    def w_rows(dz, e, kk):
        return wt.at[w_slot(dz, e), pl.ds(pl.multiple_of(kk * HR, HR), HR), :]

    def w_fwd(dz, e, kk):
        i = dz * 2 + e - 1
        ref = w_rows(dz, e, kk)
        return rcopy(ref, ref, wf_send.at[i], wf_recv.at[i], partner)

    def wx(idx, cc, half, dev):
        cols = pl.ds(0, 1024) if half is None else pl.ds(half * 512, 512)
        ref = wt.at[:, share(cc), cols]
        return rcopy(ref, ref, wx_send.at[idx], wx_recv.at[idx], dev)

    def xdev(dx):
        return {"cp": mod(x + dx, NX) * 2 + k}

    def blk(dx, kk):
        return mod(x + dx, NX) * 2 + kk

    def go(cp_):
        cp_.start()
        sends.append(cp_)

    def wx_start():
        for dz, e in group:
            i = dz * 2 + e - 1
            ref = wt.at[w_slot(dz, e), share(c), :]
            rcopy(ref, ref, sh_send.at[i], sh_recv.at[i], partner).wait_recv()
        wo_own[1].wait()
        go(wx(0, c, 0, xdev(1)))
        go(wx(1, c, 1, xdev(3)))
        go(wx(2, c, None, partner))

    def wx_second():
        go(wx(8, c, 1, xdev(1)))
        go(wx(9, c, 0, xdev(3)))

    def wx_relay():
        wx(0, blk(3, k), 0, partner).wait_recv()
        go(wx(3, blk(3, k), 0, xdev(1)))
        wx(1, blk(1, k), 1, partner).wait_recv()
        go(wx(5, blk(1, k), 1, xdev(3)))

    def wx_last():
        w_forward()
        wx(8, blk(3, k), 1, partner).wait_recv()
        go(wx(4, blk(3, k), None, partner))
        wx(9, blk(1, k), 0, partner).wait_recv()
        go(wx(6, blk(1, k), None, partner))
        wx(3, blk(2, k), 0, partner).wait_recv()
        wx(5, blk(2, k), 1, partner).wait_recv()
        go(wx(7, blk(2, k), None, partner))

    def w_forward():
        for dz, e in group:
            i = dz * 2 + e - 1
            ref = w_rows(dz, e, k)
            rcopy(ref, ref, ws_send.at[i], ws_recv.at[i], partner).wait_recv()
            go(w_fwd(dz, e, k))

    def w_done():
        wo_own[0].wait()
        for dz, e in group:
            w_fwd(dz, e, 1 - k).wait_recv()
        wx(2, blk(0, 1 - k), None, partner).wait_recv()
        wx(4, blk(3, 1 - k), None, partner).wait_recv()
        wx(6, blk(1, 1 - k), None, partner).wait_recv()
        wx(7, blk(2, 1 - k), None, partner).wait_recv()

    group = [(dz, e) for dz in range(NX) for e in range(2) if dz or e]
    def spread_w():
        pl.semaphore_wait(bar, n_peers)
        seg_own.wait()
        for dc in range(1, 2 * NX):
            cp_ = rcopy(segs.at[c], segs.at[c], sg_send.at[dc - 1], sg_recv.at[dc - 1], {"cp": mod(c + dc, 2 * NX)})
            cp_.start()
            sends.append(cp_)
        for shared in (True, False):
            for dz, e in group:
                go(w_move(dz, e, shared))
        for cp_ in reversed(wo_own):
            cp_.start()

    def project(w, lo, hi):
        def step(i, _):
            nxt = i + 2

            @pl.when(nxt < NKC // 2)
            def _():
                load(w, nxt)
            if w < 2:
                @pl.when(nxt >= NKC // 2)
                def _():
                    load(w + 1, nxt - NKC // 2)
            for b, cp_ in enumerate(w_copies(w, i)):
                cp_.wait()
                if w == 0:
                    x_copy(2 * i + b).wait()
            g = lax.rem(4 * w + i, 3) * 2
            acc[...] += (jnp.dot(xbuf[2 * i], wbuf[g], preferred_element_type=F32)
                         + jnp.dot(xbuf[2 * i + 1], wbuf[g + 1], preferred_element_type=F32))
            return 0
        lax.fori_loop(lo, hi, step, 0)

    def split(dst):
        for h in range(4):
            dst[h] = acc[:, h * HD:(h + 1) * HD].astype(BF)

    def kv_copy(n, idx, src, dst, dev):
        return rcopy(src, dst, kv_send.at[n, idx], kv_recv.at[n, idx], dev)

    def kv_spread(n, loc, gat):
        for dx in (2, 1, 3):
            go(kv_copy(n, dx - 1, loc.at[mod(x + dx, NX)], gat.at[c], xdev(dx)))
        go(kv_copy(n, 3, loc.at[x], gat.at[c], partner))
        gat[c] = loc[x]

    def kv_forward(n, gat):
        for dx in (1, 3, 2):
            ref = gat.at[blk(4 - dx, k)]
            kv_copy(n, dx - 1, ref, ref, partner).wait_recv()
            go(rcopy(ref, ref, kf_send.at[n, dx - 1], kf_recv.at[n, dx - 1], partner))

    def kv_finish(n, gat):
        ref = gat.at[blk(0, 1 - k)]
        kv_copy(n, 3, ref, ref, partner).wait_recv()
        for dx in (1, 3, 2):
            ref = gat.at[blk(4 - dx, 1 - k)]
            rcopy(ref, ref, kf_send.at[n, dx - 1], kf_recv.at[n, dx - 1], partner).wait_recv()

    acc[...] = jnp.zeros_like(acc)
    with jax.named_scope("proj_k0"):
        project(0, 0, 2)
    with jax.named_scope("barrier"):
        spread_w()
    with jax.named_scope("proj_k1"):
        project(0, 2, 4)
    split(kloc)
    acc[...] = jnp.zeros_like(acc)
    kv_spread(0, kloc, kg)
    with jax.named_scope("proj_v"):
        project(1, 0, 4)
    for h in range(4):
        vloc[h] = jnp.transpose(acc[:, h * HD:(h + 1) * HD]).astype(BF)
    acc[...] = jnp.zeros_like(acc)
    kv_spread(1, vloc, vg)
    with jax.named_scope("proj_q0"):
        project(2, 0, 2)
    with jax.named_scope("fwd_k"):
        kv_forward(0, kg)
    with jax.named_scope("proj_q1"):
        project(2, 2, 4)
    split(qloc)
    own = lax.rem(x + k, 2)
    for dx in (2, 1, 3):
        h = mod(x + dx, NX)
        cp_ = rcopy(qloc.at[h], qg.at[x], q_send.at[dx - 1], q_recv.at[x], {"cp": h * 2 + own})
        cp_.start()
        sends.append(cp_)

    @pl.when(xodd == 0)
    def _():
        qg[x] = qloc[x]

    q_d2d = rcopy(qloc.at[x], qg.at[x], q_send.at[3], q_recv.at[x], partner)

    @pl.when(xodd == 1)
    def _():
        q_d2d.start()

    with jax.named_scope("segs"):
        for dc in range(1, 2 * NX):
            ref = segs.at[mod(c - dc, 2 * NX)]
            rcopy(ref, ref, sg_send.at[dc - 1], sg_recv.at[dc - 1], partner).wait_recv()

        def seg_columns(j, _):
            sk[j] = jnp.transpose(jnp.broadcast_to(segs[j], (HD, L)))
            return 0
        lax.fori_loop(0, 2 * NX, seg_columns, 0)
    with jax.named_scope("fwd_v"):
        kv_forward(1, vg)

    with jax.named_scope("fin_kv"):
        kv_finish(0, kg)
        kv_finish(1, vg)
    tiles = [slice(b, b + HL) for b in range(0, L, HL)]

    def q_block(xx):
        return 2 * xx + lax.rem(k + xx, 2)

    def local(xx):
        return (x == xx) & (xodd == 0)

    def scores(xx, j, n, rows, diag):
        s = lax.dot_general(kg[j, 0:n, :], qg[xx, rows, :], (((1,), (1,)), ((), ())), preferred_element_type=F32)
        ok = jnp.concatenate([sk[j, 0:n, :]] * (HL // HD), axis=1) == jnp.broadcast_to(segs[q_block(xx)][:, rows], (n, HL))
        if diag:
            qi = lax.broadcasted_iota(jnp.int32, (n, HL), 1) + rows.start
            ok = ok & (lax.broadcasted_iota(jnp.int32, (n, HL), 0) <= qi)
        return jnp.where(ok, s * SCALE, -jnp.inf)

    def update(xx, blocks):
        for rows in tiles:
            ss = [scores(xx, j, L, rows, False) for j in blocks]
            m = m_s[xx, :, rows]
            m_new = m
            for s in ss:
                m_new = jnp.maximum(m_new, jnp.max(s, axis=0, keepdims=True))
            alpha = jnp.exp2(m - m_new)
            l, o = l_s[xx, :, rows] * alpha, o_s[xx, :, rows] * alpha
            for j, s in zip(blocks, ss):
                p = jnp.exp2(s - m_new)
                l += jnp.sum(p, axis=0, keepdims=True)
                o += jnp.dot(vg[j], p.astype(BF), preferred_element_type=F32)
            m_s[xx, :, rows], l_s[xx, :, rows], o_s[xx, :, rows] = m_new, l, o

    def o_ret(xx):
        ocol = pl.ds(pl.multiple_of(s_me * F + x * HD, HD), HD)
        return rcopy(obuf.at[xx], og.at[:, ocol], o_send.at[xx], o_recv.at[x], {"cp": q_block(xx)}), ocol

    def finish(xx):
        obuf[xx] = jnp.transpose(o_s[xx] / l_s[xx]).astype(BF)
        ret, ocol = o_ret(xx)

        @pl.when(local(xx))
        def _():
            og[:, ocol] = obuf[xx]

        pl.when(jnp.logical_not(local(xx)))(ret.start)

    def attend_own():
        for xx in range(NX):
            c_q = q_block(xx)
            for rows in tiles:
                s = scores(xx, c_q, rows.stop, rows, True)
                m = jnp.max(s, axis=0, keepdims=True)
                p = jnp.exp2(s - m)
                m_s[xx, :, rows] = m
                l_s[xx, :, rows] = jnp.sum(p, axis=0, keepdims=True)
                o_s[xx, :, rows] = jnp.dot(vg[c_q, :, 0:rows.stop], p.astype(BF), preferred_element_type=F32)
        for xx in (1 - k, 3 - k):
            update(xx, [2 * xx])
        finish(0)

    def attend_chip(i):
        for n in range(NX - 1 - i):
            xx = n + i + 1 if i else 1 + lax.rem(x + n, NX - 1)
            update(xx, [2 * i, 2 * i + 1])
            if i == 0:
                finish(xx)

    def wait_o():
        for h in range(NX):
            o_in = rcopy(obuf.at[0], og.at[:, pl.ds(pl.multiple_of(s_me * F + h * HD, HD), HD)], o_send.at[0], o_recv.at[h], partner)
            pl.when(jnp.logical_not((x == h) & (xodd == 0)))(o_in.wait_recv)

    with jax.named_scope("wait_q"):
        for xx in range(NX):
            pl.when(jnp.logical_not(local(xx)))(rcopy(qg.at[xx], qg.at[xx], q_send.at[3], q_recv.at[xx], partner).wait_recv)
    with jax.named_scope("wx_start"):
        wx_start()
    with jax.named_scope("attn"):
        attend_own()
    wx_second()
    with jax.named_scope("attn2"):
        attend_chip(2)
    with jax.named_scope("attn1"):
        attend_chip(1)
    with jax.named_scope("wx_relay"):
        wx_relay()
    with jax.named_scope("attn0"):
        attend_chip(0)

    def row_ds(r):
        return pl.ds(ROWS[r][0], ROWS[r][1])

    def o_copy(r, idx, zz, e, dev):
        s = zz * 2 + lax.rem(yb + e, 2)
        ref = og.at[row_ds(r), pl.ds(pl.multiple_of(s * F, F), F)]
        return rcopy(ref, ref, a_send.at[r, idx], a_recv.at[r, idx], dev)

    def o_send_z(r, e):
        d = O_DIR[r]
        go(o_copy(r, 1 + 3 * e, z, e, tpdev(mod(z + d, NX), y)))
        go(o_copy(r, 2 + 3 * e, z, e, tpdev(mod(z + NX - d, NX), y)))

    pair = tpdev(z, yh * 2 + 1 - yb)
    o_seen = []

    def ostart(r):
        if not o_seen:
            o_seen.append(r)
            with jax.named_scope("wait_o"):
                wait_o()
        go(o_copy(r, 0, z, 0, pair))
        o_send_z(r, 0)
        if len(o_seen) == 1:
            o_seen.append(r)

    def o_forward(r, e):
        d = O_DIR[r]
        zz = mod(z + NX - d, NX)
        o_copy(r, 1 + 3 * e, zz, e, partner).wait_recv()
        go(o_copy(r, 3 + 3 * e, zz, e, tpdev(mod(z + d, NX), y)))

    def o_pair(r, idx, new, zz):
        o_copy(r, idx, zz, 0, partner).wait_recv()
        go(o_copy(r, new, zz, 0, pair))

    def opair(r):
        if O_FIRST[r] == 0:
            o_pair(r, 2, 5, mod(z + O_DIR[r], NX))
            return
        o_copy(r, 0, z, 1, partner).wait_recv()
        o_send_z(r, 1)

    def ofw0(r):
        o_forward(r, 0)
        if O_FIRST[r] == 0:
            go(o_copy(r, 4, mod(z + NX - O_DIR[r], NX), 0, pair))

    def ofw1(r):
        if O_FIRST[r] == 0:
            o_pair(r, 3, 6, mod(z + 2, NX))
            return
        o_forward(r, 1)

    def o_rest(r):
        d = O_DIR[r]
        if O_FIRST[r] == 0:
            for idx, zz in ((0, z), (4, mod(z + NX - d, NX)), (5, mod(z + d, NX)), (6, mod(z + 2, NX))):
                o_copy(r, idx, zz, 1, partner).wait_recv()
            return
        for e in range(2):
            o_copy(r, 2 + 3 * e, mod(z + d, NX), e, partner).wait_recv()
            o_copy(r, 3 + 3 * e, mod(z + 2, NX), e, partner).wait_recv()

    def matmul(r, half):
        out = psend if half == 0 else pown
        hh = (1 - yh) if half == 0 else yh
        a, n = ROWS[r]
        for b in range(2):
            cols = pl.ds(pl.multiple_of(hh * F + b * 256, 256), 256)
            out[a:a + n, b * 256:(b + 1) * 256] = jnp.dot(og[a:a + n, :], wt[:, :, cols].reshape(8 * F, 256), preferred_element_type=F32)

    def rs_copy(r):
        return rcopy(psend.at[row_ds(r), :], rsb.at[row_ds(r), :], r_send.at[r], r_recv.at[r], tpdev(z, 3 - y))

    def mm0(r):
        o_rest(r)
        if r == first_mm:
            with jax.named_scope("w_done"):
                w_done()
        matmul(r, 0)
        go(rs_copy(r))

    def y_pos(r, a, b):
        if Y_ORDER[r] == 0:
            return mod(z + a, NX), mod(y + b, NX)
        return mod(z + b, NX), mod(y + a, NX)

    def y_ref(r, pos):
        return yg.at[row_ds(r), pl.ds(pl.multiple_of(piece_of(*pos) * F, F), F)]

    def y_copy(r, idx, pos, dev):
        ref = y_ref(r, pos)
        return rcopy(ref, ref, y_send.at[r, idx], y_recv.at[r, idx], dev)

    def y_second(r, j, a):
        d2 = Y_DIR[r][1]
        pos = y_pos(r, a, 0)
        go(y_copy(r, 3 + 3 * j, pos, tpdev(*y_pos(r, 0, d2))))
        go(y_copy(r, 4 + 3 * j, pos, tpdev(*y_pos(r, 0, NX - d2))))

    def yst(r):
        rs_copy(r).wait_recv()
        a, n = ROWS[r]
        yg[a:a + n, pl.ds(pl.multiple_of(piece_of(z, y) * F, F), F)] = (pown[a:a + n, :] + rsb[a:a + n, :]).astype(BF)
        d = Y_DIR[r][0]
        pos = y_pos(r, 0, 0)
        go(y_copy(r, 0, pos, tpdev(*y_pos(r, d, 0))))
        go(y_copy(r, 1, pos, tpdev(*y_pos(r, NX - d, 0))))
        y_second(r, 0, 0)

    def ym0(r):
        d = Y_DIR[r][0]
        pos = y_pos(r, NX - d, 0)
        y_copy(r, 0, pos, partner).wait_recv()
        go(y_copy(r, 2, pos, tpdev(*y_pos(r, d, 0))))
        y_second(r, 1, NX - d)

    def ym1(r):
        d = Y_DIR[r][0]
        y_copy(r, 1, y_pos(r, d, 0), partner).wait_recv()
        y_second(r, 2, d)

    def ym2(r):
        y_copy(r, 2, y_pos(r, 2, 0), partner).wait_recv()
        y_second(r, 3, 2)

    def y_offs(r):
        d = Y_DIR[r][0]
        return (0, NX - d, d, 2)

    def yf(r, j):
        d2 = Y_DIR[r][1]
        pos = y_pos(r, y_offs(r)[j], NX - d2)
        y_copy(r, 3 + 3 * j, pos, partner).wait_recv()
        go(y_copy(r, 5 + 3 * j, pos, tpdev(*y_pos(r, 0, d2))))

    def ye(r):
        d2 = Y_DIR[r][1]
        for j, a in enumerate(y_offs(r)):
            y_copy(r, 4 + 3 * j, y_pos(r, a, d2), partner).wait_recv()
            y_copy(r, 5 + 3 * j, y_pos(r, a, 2), partner).wait_recv()

    steps = dict(ostart=ostart, opair=opair, ofw0=ofw0, ofw1=ofw1, mm0=mm0,
                 mm1=lambda r: matmul(r, 1), wxl=wx_last, yst=yst, ym0=ym0, ym1=ym1, ym2=ym2, yf=yf, ye=ye)
    first_mm = [a[1] for a in ORDER if a[0] == "mm0"][0]
    for name, *args in ORDER:
        with jax.named_scope(name + "_".join(str(a) for a in args)):
            steps[name](*args)

    for cp_ in sends:
        cp_.wait_send()

    @pl.when(xodd == 1)
    def _():
        q_d2d.wait_send()

    for xx in range(NX):
        pl.when(jnp.logical_not(local(xx)))(o_ret(xx)[0].wait_send)


def solution(mesh):
    def body(x, doc, wq, wk, wv, wo):
        seg = doc.reshape(1, L)
        dma = pltpu.SemaphoreType.DMA
        any_ = pl.BlockSpec(memory_space=pl.ANY)
        return pl.pallas_call(
            kernel,
            out_shape=pltpu.VMEM((L, D), BF),
            in_specs=[any_] * 6,
            out_specs=pl.BlockSpec(memory_space=pltpu.VMEM),
            scratch_shapes=[
                pltpu.VMEM((NKC, L, KC), BF), pltpu.VMEM((NB, KC, F), BF), pltpu.VMEM((L, F), F32),
                pltpu.VMEM((4, L, HD), BF), pltpu.VMEM((4, HD, L), BF), pltpu.VMEM((4, L, HD), BF),
                pltpu.VMEM((8, L, HD), BF), pltpu.VMEM((8, HD, L), BF), pltpu.VMEM((4, L, HD), BF), pltpu.VMEM((4, L, HD), BF),
                pltpu.VMEM((L, 8 * F), BF), pltpu.VMEM((8, F, 1024), BF),
                pltpu.VMEM((L, F), F32), pltpu.VMEM((L, F), F32), pltpu.VMEM((L, F), F32),
                pltpu.VMEM((8, 1, L), jnp.int32), pltpu.VMEM((8, L, HD), jnp.int32),
                pltpu.VMEM((NX, 1, L), F32), pltpu.VMEM((NX, 1, L), F32), pltpu.VMEM((NX, HD, L), F32),
                dma((NKC,)), dma((NB,)), dma((2,)), dma((7,)), dma((7,)), dma((7,)), dma((7,)), dma((7,)), dma((7,)), dma((10,)), dma((10,)),
                dma((2, 4)), dma((2, 4)), dma((2, 3)), dma((2, 3)), dma((4,)), dma((4,)), dma((4,)), dma((4,)),
                dma((7,)), dma((7,)), dma, dma((R, 7)), dma((R, 7)), dma((R,)), dma((R,)), dma((R, 15)), dma((R, 15)),
            ],
            compiler_params=pltpu.CompilerParams(collective_id=0, has_side_effects=True, vmem_limit_bytes=50 * 1024 * 1024),
        )(x, seg, wq, wk, wv, wo)

    return jax.shard_map(body, mesh=mesh, in_specs=(P(('dp', 'cp'), None), P(('dp', 'cp')), P(None, 'tp'), P(None, 'tp'), P(None, 'tp'), P('tp', None)), out_specs=P(('dp', 'cp'), None), check_vma=False)
```

```python
import jax
import jax.numpy as jnp
from jax import lax
from jax.experimental import pallas as pl
from jax.experimental.pallas import tpu as pltpu
from jax.sharding import PartitionSpec as P

MESH = pl.DeviceIdType.MESH
HD = 128
NX = 4
L = 512
D = 8192
F = 512
KC = 1024
NKC = D // KC
NB = 6
ROWS = ((0, 64), (64, 64), (128, 128), (256, 128), (384, 64), (448, 64))
R = len(ROWS)
Y_ORDER = (0, 1, 1, 0, 1, 1)
Y_DIR = ((1, 3), (1, 1), (3, 3), (1, 1), (3, 1), (3, 3))
O_FIRST = (1, 1, 0, 0, 1, 0)
O_DIR = (1, 1, 3, 1, 3, 3)
ORDER = (
    ("ostart", 5,), ("ostart", 1,), ("ostart", 0,), ("ofw0", 5,), ("ostart", 2,), ("opair", 5,),
    ("opair", 1,), ("opair", 0,), ("ofw1", 5,), ("wxl",), ("ofw0", 1,), ("opair", 2,),
    ("ofw1", 1,), ("ofw0", 0,), ("ostart", 4,), ("ofw0", 2,), ("mm0", 5,), ("ofw0", 4,),
    ("mm1", 5,), ("ofw1", 0,), ("mm0", 1,), ("mm1", 1,), ("ofw1", 2,), ("ostart", 3,),
    ("opair", 4,), ("yst", 5,), ("mm0", 0,), ("yst", 1,), ("ofw0", 3,), ("ofw1", 4,),
    ("mm0", 2,), ("opair", 3,), ("yf", 5, 0,), ("mm1", 0,), ("ym0", 5,), ("ym0", 1,),
    ("mm0", 4,), ("ym1", 5,), ("mm1", 2,), ("mm1", 4,), ("ym1", 1,), ("ofw1", 3,),
    ("yst", 2,), ("ym2", 5,), ("yst", 4,), ("ym2", 1,), ("mm0", 3,), ("mm1", 3,),
    ("yst", 0,), ("ym1", 2,), ("ym1", 4,), ("ym0", 0,), ("ym0", 4,), ("yst", 3,),
    ("yf", 5, 3,), ("ym2", 0,), ("ym1", 0,), ("yf", 1, 2,), ("ym0", 2,), ("ym1", 3,),
    ("ym0", 3,), ("yf", 2, 0,), ("yf", 4, 1,), ("ym2", 4,), ("yf", 5, 1,), ("yf", 0, 1,),
    ("yf", 3, 2,), ("yf", 5, 2,), ("ym2", 3,), ("yf", 2, 1,), ("yf", 1, 3,), ("yf", 0, 2,),
    ("ym2", 2,), ("yf", 3, 0,), ("yf", 1, 1,), ("yf", 1, 0,), ("yf", 0, 0,), ("yf", 4, 2,),
    ("yf", 3, 3,), ("yf", 4, 0,), ("yf", 2, 2,), ("yf", 3, 1,), ("yf", 4, 3,), ("yf", 2, 3,),
    ("yf", 0, 3,), ("ye", 4,), ("ye", 0,), ("ye", 2,), ("ye", 5,), ("ye", 1,),
    ("ye", 3,),
)
HL = L // 2
SCALE = (HD ** -0.5) * 1.4426950408889634
U = 16
DR = L - 8 * U
BF = jnp.bfloat16
F32 = jnp.float32


def mod(a, n):
    return lax.rem(a + n, n)


def kernel(x_hbm, seg_hbm, wq_hbm, wk_hbm, wv_hbm, wo_hbm, yg,
           xbuf, wbuf, acc, kloc, vloc, qloc, kg, vg, qg, obuf, og, wt, psend, pown, rsb, segs, sk, m_s, l_s, o_s,
           x_sem, w_sem, wo_sem, ws_send, ws_recv, wf_send, wf_recv, sh_send, sh_recv, wx_send, wx_recv,
           kv_send, kv_recv, kf_recv, q_send, q_recv, o_send, o_recv,
           sg_send, sg_recv, sg_loc, a_send, a_recv, r_send, r_recv, y_send, y_recv):
    t = lax.axis_index("tp")
    c = lax.axis_index("cp")
    x, k = c // 2, lax.rem(c, 2)
    z, y = t // NX, lax.rem(t, NX)
    yh, yb = y // 2, lax.rem(y, 2)
    xodd = lax.rem(x, 2)
    partner = {"cp": x * 2 + 1 - k}

    def iy(yy):
        return lax.rem(yy + yy // 2, 2)

    def slice_of(zz, yy):
        return zz * 2 + iy(yy)

    def piece_of(zz, yy):
        return slice_of(zz, yy) * 2 + yy // 2

    def tpdev(zz, yy):
        return {"tp": zz * NX + yy}

    def rcopy(src, dst, ss, rs, dev):
        return pltpu.make_async_remote_copy(src_ref=src, dst_ref=dst, send_sem=ss, recv_sem=rs, device_id=dev, device_id_type=MESH)

    s_me = z * 2 + yb
    sl_me = slice_of(z, y)
    sends = []

    def x_copy(i):
        return pltpu.make_async_copy(x_hbm.at[:, pl.ds(pl.multiple_of(i * KC, KC), KC)], xbuf.at[i], x_sem.at[i])

    w_hbms = (wk_hbm, wv_hbm, wq_hbm)

    def w_copies(w, i):
        g = lax.rem(4 * w + i, 3) * 2
        return [pltpu.make_async_copy(w_hbms[w].at[pl.ds(pl.multiple_of((2 * i + b) * KC, KC), KC), :], wbuf.at[g + b], w_sem.at[g + b]) for b in range(2)]

    def load(w, i):
        for b, cp_ in enumerate(w_copies(w, i)):
            if w == 0:
                x_copy(2 * i + b).start()
            cp_.start()

    for i in range(2):
        load(0, jnp.int32(i))
    seg_own = pltpu.make_async_copy(seg_hbm, segs.at[c], sg_loc)
    seg_own.start()
    my_cols = pl.ds(pl.multiple_of(sl_me * 1024, 1024), 1024)

    def share(cc):
        return pl.ds(pl.multiple_of(DR + cc * U, 8), U)

    wo_own = [pltpu.make_async_copy(wo_hbm.at[pl.ds(0, DR), my_cols], wt.at[s_me, pl.ds(0, DR), :], wo_sem.at[0]),
              pltpu.make_async_copy(wo_hbm.at[share(c), my_cols], wt.at[s_me, share(c), :], wo_sem.at[1])]

    bar = pltpu.get_barrier_semaphore()
    n_peers = 0
    for dc in range(1, 2 * NX):
        pl.semaphore_signal(bar, inc=1, device_id={"cp": mod(c + dc, 2 * NX)}, device_id_type=MESH)
        n_peers += 1
    for dz in range(NX):
        for e in range(2):
            if dz or e:
                pl.semaphore_signal(bar, inc=1, device_id=tpdev(mod(z + dz, NX), yh * 2 + lax.rem(yb + e, 2)), device_id_type=MESH)
                n_peers += 1
    pl.semaphore_signal(bar, inc=1, device_id=tpdev(z, 3 - y), device_id_type=MESH)
    n_peers += 1

    HR = DR // 2

    def w_move(dz, e, shared):
        z2, y2 = mod(z + dz, NX), yh * 2 + lax.rem(yb + e, 2)
        i = dz * 2 + e - 1
        rows = share(c) if shared else pl.ds(pl.multiple_of(k * HR, HR), HR)
        return rcopy(wo_hbm.at[rows, pl.ds(pl.multiple_of(slice_of(z2, y2) * 1024, 1024), 1024)], wt.at[s_me, rows, :],
                     sh_send if shared else ws_send, sh_recv.at[i] if shared else ws_recv.at[i], tpdev(z2, y2))

    def w_slot(dz, e):
        return mod(z - dz, NX) * 2 + lax.rem(yb + e, 2)

    def w_rows(dz, e, kk):
        return wt.at[w_slot(dz, e), pl.ds(pl.multiple_of(kk * HR, HR), HR), :]

    def w_fwd(dz, e, kk):
        i = dz * 2 + e - 1
        ref = w_rows(dz, e, kk)
        return rcopy(ref, ref, wf_send, wf_recv.at[i], partner)

    def wx(idx, cc, half, dev):
        cols = pl.ds(0, 1024) if half is None else pl.ds(half * 512, 512)
        ref = wt.at[:, share(cc), cols]
        return rcopy(ref, ref, wx_send, wx_recv.at[idx], dev)

    def xdev(dx):
        return {"cp": mod(x + dx, NX) * 2 + k}

    def blk(dx, kk):
        return mod(x + dx, NX) * 2 + kk

    def go(cp_):
        cp_.start()

    def wx_start():
        for dz, e in group:
            i = dz * 2 + e - 1
            ref = wt.at[w_slot(dz, e), share(c), :]
            rcopy(ref, ref, sh_send, sh_recv.at[i], partner).wait_recv()
        wo_own[1].wait()
        go(wx(0, c, 0, xdev(1)))
        go(wx(1, c, 1, xdev(3)))
        go(wx(2, c, None, partner))

    def wx_second():
        go(wx(8, c, 1, xdev(1)))
        go(wx(9, c, 0, xdev(3)))

    def wx_relay():
        wx(0, blk(3, k), 0, partner).wait_recv()
        go(wx(3, blk(3, k), 0, xdev(1)))
        wx(1, blk(1, k), 1, partner).wait_recv()
        go(wx(5, blk(1, k), 1, xdev(3)))

    def wx_last():
        w_forward((2,))
        wx(8, blk(3, k), 1, partner).wait_recv()
        go(wx(4, blk(3, k), None, partner))
        wx(9, blk(1, k), 0, partner).wait_recv()
        go(wx(6, blk(1, k), None, partner))
        wx(3, blk(2, k), 0, partner).wait_recv()
        wx(5, blk(2, k), 1, partner).wait_recv()
        go(wx(7, blk(2, k), None, partner))

    def w_forward(dzs):
        for dz, e in [g for g in group if g[0] in dzs]:
            i = dz * 2 + e - 1
            ref = w_rows(dz, e, k)
            rcopy(ref, ref, ws_send, ws_recv.at[i], partner).wait_recv()
            go(w_fwd(dz, e, k))

    def w_done():
        wo_own[0].wait()
        for dz, e in group:
            w_fwd(dz, e, 1 - k).wait_recv()
        wx(2, blk(0, 1 - k), None, partner).wait_recv()
        wx(4, blk(3, 1 - k), None, partner).wait_recv()
        wx(6, blk(1, 1 - k), None, partner).wait_recv()
        wx(7, blk(2, 1 - k), None, partner).wait_recv()

    group = [(dz, e) for dz in range(NX) for e in range(2) if dz or e]
    def spread_w():
        pl.semaphore_wait(bar, n_peers)
        seg_own.wait()
        for dc in range(1, 2 * NX):
            cp_ = rcopy(segs.at[c], segs.at[c], sg_send, sg_recv.at[dc - 1], {"cp": mod(c + dc, 2 * NX)})
            cp_.start()
        for shared in (True, False):
            for dz, e in group:
                go(w_move(dz, e, shared))
        for cp_ in reversed(wo_own):
            cp_.start()

    def project(w, lo, hi):
        def step(i, _):
            nxt = i + 2

            @pl.when(nxt < NKC // 2)
            def _():
                load(w, nxt)
            if w < 2:
                @pl.when(nxt >= NKC // 2)
                def _():
                    load(w + 1, nxt - NKC // 2)
            for b, cp_ in enumerate(w_copies(w, i)):
                cp_.wait()
                if w == 0:
                    x_copy(2 * i + b).wait()
            g = lax.rem(4 * w + i, 3) * 2
            acc[...] += (jnp.dot(xbuf[2 * i], wbuf[g], preferred_element_type=F32)
                         + jnp.dot(xbuf[2 * i + 1], wbuf[g + 1], preferred_element_type=F32))
            return 0
        lax.fori_loop(lo, hi, step, 0)

    def split(dst):
        for h in range(4):
            dst[h] = acc[:, h * HD:(h + 1) * HD].astype(BF)

    def kv_copy(n, idx, src, dst, dev):
        return rcopy(src, dst, kv_send.at[n], kv_recv.at[n, idx], dev)

    def kv_spread(n, loc, gat):
        for dx in (2, 1, 3):
            go(kv_copy(n, dx - 1, loc.at[mod(x + dx, NX)], gat.at[c], xdev(dx)))
        go(kv_copy(n, 3, loc.at[x], gat.at[c], partner))
        gat[c] = loc[x]

    def kv_forward(n, gat):
        for dx in (1, 3, 2):
            ref = gat.at[blk(4 - dx, k)]
            kv_copy(n, dx - 1, ref, ref, partner).wait_recv()
            go(rcopy(ref, ref, kv_send.at[n], kf_recv.at[n, dx - 1], partner))

    def kv_partner(n, gat):
        ref = gat.at[blk(0, 1 - k)]
        kv_copy(n, 3, ref, ref, partner).wait_recv()

    def kv_finish(n, gat):
        for dx in (1, 3, 2):
            ref = gat.at[blk(4 - dx, 1 - k)]
            rcopy(ref, ref, kv_send.at[n], kf_recv.at[n, dx - 1], partner).wait_recv()

    acc[...] = jnp.zeros_like(acc)
    with jax.named_scope("proj_k0"):
        project(0, 0, 2)
    with jax.named_scope("barrier"):
        spread_w()
    with jax.named_scope("proj_k1"):
        project(0, 2, 4)
    split(kloc)
    acc[...] = jnp.zeros_like(acc)
    kv_spread(0, kloc, kg)
    with jax.named_scope("proj_v"):
        project(1, 0, 4)
    for h in range(4):
        vloc[h] = jnp.transpose(acc[:, h * HD:(h + 1) * HD]).astype(BF)
    acc[...] = jnp.zeros_like(acc)
    kv_spread(1, vloc, vg)
    with jax.named_scope("proj_q0"):
        project(2, 0, 2)
    with jax.named_scope("fwd_k"):
        kv_forward(0, kg)
    with jax.named_scope("proj_q1"):
        project(2, 2, 4)
    split(qloc)
    own = lax.rem(x + k, 2)
    for dx in (2, 1, 3):
        h = mod(x + dx, NX)
        cp_ = rcopy(qloc.at[h], qg.at[x], q_send.at[dx - 1], q_recv.at[x], {"cp": h * 2 + own})
        cp_.start()
        sends.append(cp_)

    @pl.when(xodd == 0)
    def _():
        qg[x] = qloc[x]

    q_d2d = rcopy(qloc.at[x], qg.at[x], q_send.at[3], q_recv.at[x], partner)

    @pl.when(xodd == 1)
    def _():
        q_d2d.start()

    with jax.named_scope("segs"):
        for dc in range(1, 2 * NX):
            ref = segs.at[mod(c - dc, 2 * NX)]
            rcopy(ref, ref, sg_send, sg_recv.at[dc - 1], partner).wait_recv()

        def seg_columns(j, _):
            sk[j] = jnp.transpose(jnp.broadcast_to(segs[j], (HD, L)))
            return 0
        lax.fori_loop(0, 2 * NX, seg_columns, 0)
    tiles = [slice(b, b + HL) for b in range(0, L, HL)]

    def q_block(xx):
        return 2 * xx + lax.rem(k + xx, 2)

    def local(xx):
        return (x == xx) & (xodd == 0)

    def scores(xx, j, n, rows, diag):
        s = lax.dot_general(kg[j, 0:n, :], qg[xx, rows, :], (((1,), (1,)), ((), ())), preferred_element_type=F32)
        ok = jnp.concatenate([sk[j, 0:n, :]] * (HL // HD), axis=1) == jnp.broadcast_to(segs[q_block(xx)][:, rows], (n, HL))
        if diag:
            qi = lax.broadcasted_iota(jnp.int32, (n, HL), 1) + rows.start
            ok = ok & (lax.broadcasted_iota(jnp.int32, (n, HL), 0) <= qi)
        return jnp.where(ok, s * SCALE, -jnp.inf)

    def update(xx, blocks):
        for rows in tiles:
            ss = [scores(xx, j, L, rows, False) for j in blocks]
            m = m_s[xx, :, rows]
            m_new = m
            for s in ss:
                m_new = jnp.maximum(m_new, jnp.max(s, axis=0, keepdims=True))
            alpha = jnp.exp2(m - m_new)
            l, o = l_s[xx, :, rows] * alpha, o_s[xx, :, rows] * alpha
            for j, s in zip(blocks, ss):
                p = jnp.exp2(s - m_new)
                l += jnp.sum(p, axis=0, keepdims=True)
                o += jnp.dot(vg[j], p.astype(BF), preferred_element_type=F32)
            m_s[xx, :, rows], l_s[xx, :, rows], o_s[xx, :, rows] = m_new, l, o

    def o_ret(xx):
        ocol = pl.ds(pl.multiple_of(s_me * F + x * HD, HD), HD)
        return rcopy(obuf.at[xx], og.at[:, ocol], o_send.at[xx], o_recv.at[x], {"cp": q_block(xx)}), ocol

    def finish(xx):
        obuf[xx] = jnp.transpose(o_s[xx] / l_s[xx]).astype(BF)
        ret, ocol = o_ret(xx)

        @pl.when(local(xx))
        def _():
            og[:, ocol] = obuf[xx]

        pl.when(jnp.logical_not(local(xx)))(ret.start)

    def q_in(a):
        xx = mod(x + a, NX)
        return rcopy(qg.at[xx], qg.at[xx], q_send.at[3], q_recv.at[xx], partner)

    def attend_own(a):
        xx = mod(x + a, NX)
        c_q = q_block(xx)
        for rows in tiles:
            s = scores(xx, c_q, rows.stop, rows, True)
            m = jnp.max(s, axis=0, keepdims=True)
            p = jnp.exp2(s - m)
            m_s[xx, :, rows] = m
            l_s[xx, :, rows] = jnp.sum(p, axis=0, keepdims=True)
            o_s[xx, :, rows] = jnp.dot(vg[c_q, :, 0:rows.stop], p.astype(BF), preferred_element_type=F32)

    def attend_before(xx):
        def chip_step(i, _):
            update(xx, [2 * i, 2 * i + 1])
            return 0
        lax.fori_loop(0, xx, chip_step, 0)
        finish(xx)

    def wait_o():
        for h in range(NX):
            o_in = rcopy(obuf.at[0], og.at[:, pl.ds(pl.multiple_of(s_me * F + h * HD, HD), HD)], o_send.at[0], o_recv.at[h], partner)
            pl.when(jnp.logical_not((x == h) & (xodd == 0)))(o_in.wait_recv)

    with jax.named_scope("own0"):
        kv_partner(0, kg)
        kv_partner(1, vg)
        pl.when(xodd == 1)(q_in(0).wait_recv)
        attend_own(0)
    with jax.named_scope("fwd_v"):
        kv_forward(1, vg)

    with jax.named_scope("fin_kv"):
        kv_finish(0, kg)
        kv_finish(1, vg)
    with jax.named_scope("own1"):
        q_in(1).wait_recv()
        q_in(3).wait_recv()
        wx_start()
        attend_own(1)
        attend_own(3)
        wx_second()
    with jax.named_scope("own2"):
        q_in(2).wait_recv()
        attend_own(2)
        for xx in (1 - k, 3 - k):
            update(xx, [2 * xx])
    for a in (2, 3, 1, 0):
        with jax.named_scope("attn%d" % a):
            attend_before(mod(x + a, NX))
    def row_ds(r):
        return pl.ds(ROWS[r][0], ROWS[r][1])

    def o_copy(r, idx, zz, e, dev):
        s = zz * 2 + lax.rem(yb + e, 2)
        ref = og.at[row_ds(r), pl.ds(pl.multiple_of(s * F, F), F)]
        return rcopy(ref, ref, a_send, a_recv.at[r, idx], dev)

    def o_send_z(r, e):
        d = O_DIR[r]
        go(o_copy(r, 1 + 3 * e, z, e, tpdev(mod(z + d, NX), y)))
        go(o_copy(r, 2 + 3 * e, z, e, tpdev(mod(z + NX - d, NX), y)))

    pair = tpdev(z, yh * 2 + 1 - yb)
    o_seen = []

    def ostart(r):
        if not o_seen:
            o_seen.append(r)
            with jax.named_scope("wait_o"):
                wait_o()
        go(o_copy(r, 0, z, 0, pair))
        o_send_z(r, 0)
        if len(o_seen) == 1:
            o_seen.append(r)
            wx_relay()
            w_forward((0, 1, 3))

    def o_forward(r, e):
        d = O_DIR[r]
        zz = mod(z + NX - d, NX)
        o_copy(r, 1 + 3 * e, zz, e, partner).wait_recv()
        go(o_copy(r, 3 + 3 * e, zz, e, tpdev(mod(z + d, NX), y)))

    def o_pair(r, idx, new, zz):
        o_copy(r, idx, zz, 0, partner).wait_recv()
        go(o_copy(r, new, zz, 0, pair))

    def opair(r):
        if O_FIRST[r] == 0:
            o_pair(r, 2, 5, mod(z + O_DIR[r], NX))
            return
        o_copy(r, 0, z, 1, partner).wait_recv()
        o_send_z(r, 1)

    def ofw0(r):
        o_forward(r, 0)
        if O_FIRST[r] == 0:
            go(o_copy(r, 4, mod(z + NX - O_DIR[r], NX), 0, pair))

    def ofw1(r):
        if O_FIRST[r] == 0:
            o_pair(r, 3, 6, mod(z + 2, NX))
            return
        o_forward(r, 1)

    def o_rest(r):
        d = O_DIR[r]
        if O_FIRST[r] == 0:
            for idx, zz in ((0, z), (4, mod(z + NX - d, NX)), (5, mod(z + d, NX)), (6, mod(z + 2, NX))):
                o_copy(r, idx, zz, 1, partner).wait_recv()
            return
        for e in range(2):
            o_copy(r, 2 + 3 * e, mod(z + d, NX), e, partner).wait_recv()
            o_copy(r, 3 + 3 * e, mod(z + 2, NX), e, partner).wait_recv()

    def matmul(r, half):
        out = psend if half == 0 else pown
        hh = (1 - yh) if half == 0 else yh
        a, n = ROWS[r]
        for b in range(2):
            cols = pl.ds(pl.multiple_of(hh * F + b * 256, 256), 256)
            out[a:a + n, b * 256:(b + 1) * 256] = jnp.dot(og[a:a + n, :], wt[:, :, cols].reshape(8 * F, 256), preferred_element_type=F32)

    def rs_copy(r):
        return rcopy(psend.at[row_ds(r), :], rsb.at[row_ds(r), :], r_send, r_recv.at[r], tpdev(z, 3 - y))

    def mm0(r):
        o_rest(r)
        if r == first_mm:
            with jax.named_scope("w_done"):
                w_done()
        matmul(r, 0)
        go(rs_copy(r))

    def y_pos(r, a, b):
        if Y_ORDER[r] == 0:
            return mod(z + a, NX), mod(y + b, NX)
        return mod(z + b, NX), mod(y + a, NX)

    def y_ref(r, pos):
        return yg.at[row_ds(r), pl.ds(pl.multiple_of(piece_of(*pos) * F, F), F)]

    def y_copy(r, idx, pos, dev):
        ref = y_ref(r, pos)
        return rcopy(ref, ref, y_send, y_recv.at[r, idx], dev)

    def y_second(r, j, a):
        d2 = Y_DIR[r][1]
        pos = y_pos(r, a, 0)
        go(y_copy(r, 3 + 3 * j, pos, tpdev(*y_pos(r, 0, d2))))
        go(y_copy(r, 4 + 3 * j, pos, tpdev(*y_pos(r, 0, NX - d2))))

    def yst(r):
        rs_copy(r).wait_recv()
        a, n = ROWS[r]
        yg[a:a + n, pl.ds(pl.multiple_of(piece_of(z, y) * F, F), F)] = (pown[a:a + n, :] + rsb[a:a + n, :]).astype(BF)
        d = Y_DIR[r][0]
        pos = y_pos(r, 0, 0)
        go(y_copy(r, 0, pos, tpdev(*y_pos(r, d, 0))))
        go(y_copy(r, 1, pos, tpdev(*y_pos(r, NX - d, 0))))
        y_second(r, 0, 0)

    def ym0(r):
        d = Y_DIR[r][0]
        pos = y_pos(r, NX - d, 0)
        y_copy(r, 0, pos, partner).wait_recv()
        go(y_copy(r, 2, pos, tpdev(*y_pos(r, d, 0))))
        y_second(r, 1, NX - d)

    def ym1(r):
        d = Y_DIR[r][0]
        y_copy(r, 1, y_pos(r, d, 0), partner).wait_recv()
        y_second(r, 2, d)

    def ym2(r):
        y_copy(r, 2, y_pos(r, 2, 0), partner).wait_recv()
        y_second(r, 3, 2)

    def y_offs(r):
        d = Y_DIR[r][0]
        return (0, NX - d, d, 2)

    def yf(r, j):
        d2 = Y_DIR[r][1]
        pos = y_pos(r, y_offs(r)[j], NX - d2)
        y_copy(r, 3 + 3 * j, pos, partner).wait_recv()
        go(y_copy(r, 5 + 3 * j, pos, tpdev(*y_pos(r, 0, d2))))

    def ye(r):
        d2 = Y_DIR[r][1]
        for j, a in enumerate(y_offs(r)):
            y_copy(r, 4 + 3 * j, y_pos(r, a, d2), partner).wait_recv()
            y_copy(r, 5 + 3 * j, y_pos(r, a, 2), partner).wait_recv()

    steps = dict(ostart=ostart, opair=opair, ofw0=ofw0, ofw1=ofw1, mm0=mm0,
                 mm1=lambda r: matmul(r, 1), wxl=wx_last, yst=yst, ym0=ym0, ym1=ym1, ym2=ym2, yf=yf, ye=ye)
    first_mm = [a[1] for a in ORDER if a[0] == "mm0"][0]
    def drain(ref, sem):
        rcopy(ref, ref, sem, r_recv.at[0], partner).wait_send()

    def drain_early():
        drain(segs.at[pl.ds(0, 7)], sg_send)
        drain(kg.at[pl.ds(0, 7)], kv_send.at[0])
        drain(vg.at[pl.ds(0, 7)], kv_send.at[1])
        drain(wt.at[pl.ds(0, 7), pl.ds(0, HR), :], ws_send)
        drain(wt.at[pl.ds(0, 7), pl.ds(0, U), :], sh_send)
        drain(wt.at[pl.ds(0, 7), pl.ds(0, HR), :], wf_send)
        drain(wt.at[:, pl.ds(0, 7 * U), :], wx_send)
        for cp_ in sends:
            cp_.wait_send()

        @pl.when(xodd == 1)
        def _():
            q_d2d.wait_send()

        for xx in range(NX):
            pl.when(jnp.logical_not(local(xx)))(o_ret(xx)[0].wait_send)

    last_y = [a[1] for a in ORDER if a[0] == "yst"][-1]
    for name, *args in ORDER:
        with jax.named_scope(name + "_".join(str(a) for a in args)):
            steps[name](*args)
        if name == "yst" and args[0] == last_y:
            drain_early()

    drain(psend, r_send)
    drain(og.at[:, pl.ds(0, 7 * F)], a_send)
    drain(yg.at[:, pl.ds(0, 15 * F)], y_send)


def solution(mesh):
    def body(x, doc, wq, wk, wv, wo):
        seg = doc.reshape(1, L)
        dma = pltpu.SemaphoreType.DMA
        any_ = pl.BlockSpec(memory_space=pl.ANY)
        return pl.pallas_call(
            kernel,
            out_shape=pltpu.VMEM((L, D), BF),
            in_specs=[any_] * 6,
            out_specs=pl.BlockSpec(memory_space=pltpu.VMEM),
            scratch_shapes=[
                pltpu.VMEM((NKC, L, KC), BF), pltpu.VMEM((NB, KC, F), BF), pltpu.VMEM((L, F), F32),
                pltpu.VMEM((4, L, HD), BF), pltpu.VMEM((4, HD, L), BF), pltpu.VMEM((4, L, HD), BF),
                pltpu.VMEM((8, L, HD), BF), pltpu.VMEM((8, HD, L), BF), pltpu.VMEM((4, L, HD), BF), pltpu.VMEM((4, L, HD), BF),
                pltpu.VMEM((L, 8 * F), BF), pltpu.VMEM((8, F, 1024), BF),
                pltpu.VMEM((L, F), F32), pltpu.VMEM((L, F), F32), pltpu.VMEM((L, F), F32),
                pltpu.VMEM((8, 1, L), jnp.int32), pltpu.VMEM((8, L, HD), jnp.int32),
                pltpu.VMEM((NX, 1, L), F32), pltpu.VMEM((NX, 1, L), F32), pltpu.VMEM((NX, HD, L), F32),
                dma((NKC,)), dma((NB,)), dma((2,)), dma, dma((7,)), dma, dma((7,)), dma, dma((7,)), dma, dma((10,)),
                dma((2,)), dma((2, 4)), dma((2, 3)), dma((4,)), dma((4,)), dma((4,)), dma((4,)),
                dma, dma((7,)), dma, dma, dma((R, 7)), dma, dma((R,)), dma, dma((R, 15)),
            ],
            compiler_params=pltpu.CompilerParams(collective_id=0, has_side_effects=True, vmem_limit_bytes=50 * 1024 * 1024),
        )(x, seg, wq, wk, wv, wo)

    return jax.shard_map(body, mesh=mesh, in_specs=(P(('dp', 'cp'), None), P(('dp', 'cp')), P(None, 'tp'), P(None, 'tp'), P(None, 'tp'), P('tp', None)), out_specs=P(('dp', 'cp'), None), check_vma=False)
```

```python
import jax
import jax.numpy as jnp
from jax import lax
from jax.experimental import pallas as pl
from jax.experimental.pallas import tpu as pltpu
from jax.sharding import PartitionSpec as P

MESH = pl.DeviceIdType.MESH
HD = 128
NX = 4
L = 512
D = 8192
F = 512
KC = 1024
NKC = D // KC
NB = 6
ROWS = ((0, 64), (64, 64), (128, 128), (256, 128), (384, 64), (448, 64))
R = len(ROWS)
Y_ORDER = (0, 1, 1, 0, 1, 1)
Y_DIR = ((1, 3), (1, 1), (3, 3), (1, 1), (3, 1), (3, 3))
O_FIRST = (1, 1, 0, 0, 1, 0)
O_DIR = (1, 1, 3, 1, 3, 3)
ORDER = (
    ("ostart", 5,), ("ostart", 1,), ("ostart", 0,), ("ofw0", 5,), ("ostart", 2,), ("opair", 5,),
    ("opair", 1,), ("opair", 0,), ("ofw1", 5,), ("wxl",), ("ofw0", 1,), ("opair", 2,),
    ("ofw1", 1,), ("ofw0", 0,), ("ostart", 4,), ("ofw0", 2,), ("mm0", 5,), ("ofw0", 4,),
    ("mm1", 5,), ("ofw1", 0,), ("mm0", 1,), ("mm1", 1,), ("ofw1", 2,), ("ostart", 3,),
    ("opair", 4,), ("yst", 5,), ("mm0", 0,), ("yst", 1,), ("ofw0", 3,), ("ofw1", 4,),
    ("mm0", 2,), ("opair", 3,), ("yf", 5, 0,), ("mm1", 0,), ("ym0", 5,), ("ym0", 1,),
    ("mm0", 4,), ("ym1", 5,), ("mm1", 2,), ("mm1", 4,), ("ym1", 1,), ("ofw1", 3,),
    ("yst", 2,), ("ym2", 5,), ("yst", 4,), ("ym2", 1,), ("mm0", 3,), ("mm1", 3,),
    ("yst", 0,), ("ym1", 2,), ("ym1", 4,), ("ym0", 0,), ("ym0", 4,), ("yst", 3,),
    ("yf", 5, 3,), ("ym2", 0,), ("ym1", 0,), ("yf", 1, 2,), ("ym0", 2,), ("ym1", 3,),
    ("ym0", 3,), ("yf", 2, 0,), ("yf", 4, 1,), ("ym2", 4,), ("yf", 5, 1,), ("yf", 0, 1,),
    ("yf", 3, 2,), ("yf", 5, 2,), ("ym2", 3,), ("yf", 2, 1,), ("yf", 1, 3,), ("yf", 0, 2,),
    ("ym2", 2,), ("yf", 3, 0,), ("yf", 1, 1,), ("yf", 1, 0,), ("yf", 0, 0,), ("yf", 4, 2,),
    ("yf", 3, 3,), ("yf", 4, 0,), ("yf", 2, 2,), ("yf", 3, 1,), ("yf", 4, 3,), ("yf", 2, 3,),
    ("yf", 0, 3,), ("ye", 4,), ("ye", 0,), ("ye", 2,), ("ye", 5,), ("ye", 1,),
    ("ye", 3,),
)
HL = L // 2
SCALE = (HD ** -0.5) * 1.4426950408889634
U = 16
DR = L - 8 * U
BF = jnp.bfloat16
F32 = jnp.float32


def mod(a, n):
    return lax.rem(a + n, n)


def kernel(x_hbm, seg_hbm, wq_hbm, wk_hbm, wv_hbm, wo_hbm, yg,
           xbuf, wbuf, acc, kloc, vloc, qloc, kg, vg, qg, obuf, og, wt, psend, pown, rsb, segs, sk, m_s, l_s, o_s,
           x_sem, w_sem, wo_sem, ws_send, ws_recv, wf_send, wf_recv, sh_send, sh_recv, wx_send, wx_recv,
           kv_send, kv_recv, kf_recv, q_send, q_recv, o_send, o_recv,
           sg_send, sg_recv, sg_loc, a_send, a_recv, r_send, r_recv, y_send, y_recv):
    t = lax.axis_index("tp")
    c = lax.axis_index("cp")
    x, k = c // 2, lax.rem(c, 2)
    z, y = t // NX, lax.rem(t, NX)
    yh, yb = y // 2, lax.rem(y, 2)
    xodd = lax.rem(x, 2)
    partner = {"cp": x * 2 + 1 - k}

    def iy(yy):
        return lax.rem(yy + yy // 2, 2)

    def slice_of(zz, yy):
        return zz * 2 + iy(yy)

    def piece_of(zz, yy):
        return slice_of(zz, yy) * 2 + yy // 2

    def tpdev(zz, yy):
        return {"tp": zz * NX + yy}

    def rcopy(src, dst, ss, rs, dev):
        return pltpu.make_async_remote_copy(src_ref=src, dst_ref=dst, send_sem=ss, recv_sem=rs, device_id=dev, device_id_type=MESH)

    s_me = z * 2 + yb
    sl_me = slice_of(z, y)
    sends = []

    def x_copy(i):
        return pltpu.make_async_copy(x_hbm.at[:, pl.ds(pl.multiple_of(i * KC, KC), KC)], xbuf.at[i], x_sem.at[i])

    w_hbms = (wk_hbm, wv_hbm, wq_hbm)

    def w_copies(w, i):
        g = lax.rem(4 * w + i, 3) * 2
        return [pltpu.make_async_copy(w_hbms[w].at[pl.ds(pl.multiple_of((2 * i + b) * KC, KC), KC), :], wbuf.at[g + b], w_sem.at[g + b]) for b in range(2)]

    def load(w, i):
        for b, cp_ in enumerate(w_copies(w, i)):
            if w == 0:
                x_copy(2 * i + b).start()
            cp_.start()

    for i in range(2):
        load(0, jnp.int32(i))
    seg_own = pltpu.make_async_copy(seg_hbm, segs.at[c], sg_loc)
    seg_own.start()
    my_cols = pl.ds(pl.multiple_of(sl_me * 1024, 1024), 1024)

    def share(cc):
        return pl.ds(pl.multiple_of(DR + cc * U, 8), U)

    wo_own = [pltpu.make_async_copy(wo_hbm.at[pl.ds(0, DR), my_cols], wt.at[s_me, pl.ds(0, DR), :], wo_sem.at[0]),
              pltpu.make_async_copy(wo_hbm.at[share(c), my_cols], wt.at[s_me, share(c), :], wo_sem.at[1])]

    bar = pltpu.get_barrier_semaphore()
    n_peers = 0
    for dc in range(1, 2 * NX):
        pl.semaphore_signal(bar, inc=1, device_id={"cp": mod(c + dc, 2 * NX)}, device_id_type=MESH)
        n_peers += 1
    for dz in range(NX):
        for e in range(2):
            if dz or e:
                pl.semaphore_signal(bar, inc=1, device_id=tpdev(mod(z + dz, NX), yh * 2 + lax.rem(yb + e, 2)), device_id_type=MESH)
                n_peers += 1
    pl.semaphore_signal(bar, inc=1, device_id=tpdev(z, 3 - y), device_id_type=MESH)
    n_peers += 1

    HR = DR // 2

    def w_move(dz, e, shared):
        z2, y2 = mod(z + dz, NX), yh * 2 + lax.rem(yb + e, 2)
        i = dz * 2 + e - 1
        rows = share(c) if shared else pl.ds(pl.multiple_of(k * HR, HR), HR)
        return rcopy(wo_hbm.at[rows, pl.ds(pl.multiple_of(slice_of(z2, y2) * 1024, 1024), 1024)], wt.at[s_me, rows, :],
                     sh_send if shared else ws_send, sh_recv.at[i] if shared else ws_recv.at[i], tpdev(z2, y2))

    def w_slot(dz, e):
        return mod(z - dz, NX) * 2 + lax.rem(yb + e, 2)

    def w_rows(dz, e, kk):
        return wt.at[w_slot(dz, e), pl.ds(pl.multiple_of(kk * HR, HR), HR), :]

    def w_fwd(dz, e, kk):
        i = dz * 2 + e - 1
        ref = w_rows(dz, e, kk)
        return rcopy(ref, ref, wf_send, wf_recv.at[i], partner)

    def wx(idx, cc, half, dev):
        cols = pl.ds(0, 1024) if half is None else pl.ds(half * 512, 512)
        ref = wt.at[:, share(cc), cols]
        return rcopy(ref, ref, wx_send, wx_recv.at[idx], dev)

    def xdev(dx):
        return {"cp": mod(x + dx, NX) * 2 + k}

    def blk(dx, kk):
        return mod(x + dx, NX) * 2 + kk

    def go(cp_):
        cp_.start()

    def wx_start():
        for dz, e in group:
            i = dz * 2 + e - 1
            ref = wt.at[w_slot(dz, e), share(c), :]
            rcopy(ref, ref, sh_send, sh_recv.at[i], partner).wait_recv()
        wo_own[1].wait()
        go(wx(0, c, 0, xdev(1)))
        go(wx(1, c, 1, xdev(3)))
        go(wx(2, c, None, partner))

    def wx_second():
        go(wx(8, c, 1, xdev(1)))
        go(wx(9, c, 0, xdev(3)))

    def wx_relay():
        wx(0, blk(3, k), 0, partner).wait_recv()
        go(wx(3, blk(3, k), 0, xdev(1)))
        wx(1, blk(1, k), 1, partner).wait_recv()
        go(wx(5, blk(1, k), 1, xdev(3)))

    def wx_last():
        w_forward((2,))
        wx(8, blk(3, k), 1, partner).wait_recv()
        go(wx(4, blk(3, k), None, partner))
        wx(9, blk(1, k), 0, partner).wait_recv()
        go(wx(6, blk(1, k), None, partner))
        wx(3, blk(2, k), 0, partner).wait_recv()
        wx(5, blk(2, k), 1, partner).wait_recv()
        go(wx(7, blk(2, k), None, partner))

    def w_forward(dzs):
        for dz, e in [g for g in group if g[0] in dzs]:
            i = dz * 2 + e - 1
            ref = w_rows(dz, e, k)
            rcopy(ref, ref, ws_send, ws_recv.at[i], partner).wait_recv()
            go(w_fwd(dz, e, k))

    def w_done():
        wo_own[0].wait()
        for dz, e in group:
            w_fwd(dz, e, 1 - k).wait_recv()
        wx(2, blk(0, 1 - k), None, partner).wait_recv()
        wx(4, blk(3, 1 - k), None, partner).wait_recv()
        wx(6, blk(1, 1 - k), None, partner).wait_recv()
        wx(7, blk(2, 1 - k), None, partner).wait_recv()

    group = [(dz, e) for dz in range(NX) for e in range(2) if dz or e]
    def spread_w():
        pl.semaphore_wait(bar, n_peers)
        seg_own.wait()
        for dc in range(1, 2 * NX):
            cp_ = rcopy(segs.at[c], segs.at[c], sg_send, sg_recv.at[dc - 1], {"cp": mod(c + dc, 2 * NX)})
            cp_.start()
        for shared in (True, False):
            for dz, e in sorted(group, key=lambda g: g[0] != 2):
                go(w_move(dz, e, shared))
        for cp_ in reversed(wo_own):
            cp_.start()

    def project(w, lo, hi):
        def step(i, _):
            nxt = i + 2

            @pl.when(nxt < NKC // 2)
            def _():
                load(w, nxt)
            if w < 2:
                @pl.when(nxt >= NKC // 2)
                def _():
                    load(w + 1, nxt - NKC // 2)
            for b, cp_ in enumerate(w_copies(w, i)):
                cp_.wait()
                if w == 0:
                    x_copy(2 * i + b).wait()
            g = lax.rem(4 * w + i, 3) * 2
            acc[...] += (jnp.dot(xbuf[2 * i], wbuf[g], preferred_element_type=F32)
                         + jnp.dot(xbuf[2 * i + 1], wbuf[g + 1], preferred_element_type=F32))
            return 0
        lax.fori_loop(lo, hi, step, 0)

    def split(dst):
        for h in range(4):
            dst[h] = acc[:, h * HD:(h + 1) * HD].astype(BF)

    def kv_copy(n, idx, src, dst, dev):
        return rcopy(src, dst, kv_send.at[n], kv_recv.at[n, idx], dev)

    def kv_spread(n, loc, gat):
        for dx in (2, 1, 3):
            go(kv_copy(n, dx - 1, loc.at[mod(x + dx, NX)], gat.at[c], xdev(dx)))
        go(kv_copy(n, 3, loc.at[x], gat.at[c], partner))
        gat[c] = loc[x]

    def kv_forward(n, gat):
        for dx in (1, 3, 2):
            ref = gat.at[blk(4 - dx, k)]
            kv_copy(n, dx - 1, ref, ref, partner).wait_recv()
            go(rcopy(ref, ref, kv_send.at[n], kf_recv.at[n, dx - 1], partner))

    def kv_partner(n, gat):
        ref = gat.at[blk(0, 1 - k)]
        kv_copy(n, 3, ref, ref, partner).wait_recv()

    def kv_finish(n, gat):
        for dx in (1, 3, 2):
            ref = gat.at[blk(4 - dx, 1 - k)]
            rcopy(ref, ref, kv_send.at[n], kf_recv.at[n, dx - 1], partner).wait_recv()

    acc[...] = jnp.zeros_like(acc)
    with jax.named_scope("proj_k0"):
        project(0, 0, 2)
    with jax.named_scope("barrier"):
        spread_w()
    with jax.named_scope("proj_k1"):
        project(0, 2, 4)
    split(kloc)
    acc[...] = jnp.zeros_like(acc)
    kv_spread(0, kloc, kg)
    with jax.named_scope("proj_v"):
        project(1, 0, 4)
    for h in range(4):
        vloc[h] = jnp.transpose(acc[:, h * HD:(h + 1) * HD]).astype(BF)
    acc[...] = jnp.zeros_like(acc)
    kv_spread(1, vloc, vg)
    with jax.named_scope("proj_q0"):
        project(2, 0, 2)
    with jax.named_scope("fwd_k"):
        kv_forward(0, kg)
    with jax.named_scope("proj_q1"):
        project(2, 2, 4)
    split(qloc)
    own = lax.rem(x + k, 2)
    for dx in (2, 1, 3):
        h = mod(x + dx, NX)
        cp_ = rcopy(qloc.at[h], qg.at[x], q_send.at[dx - 1], q_recv.at[x], {"cp": h * 2 + own})
        cp_.start()
        sends.append(cp_)

    @pl.when(xodd == 0)
    def _():
        qg[x] = qloc[x]

    q_d2d = rcopy(qloc.at[x], qg.at[x], q_send.at[3], q_recv.at[x], partner)

    @pl.when(xodd == 1)
    def _():
        q_d2d.start()

    with jax.named_scope("segs"):
        for dc in range(1, 2 * NX):
            ref = segs.at[mod(c - dc, 2 * NX)]
            rcopy(ref, ref, sg_send, sg_recv.at[dc - 1], partner).wait_recv()

        def seg_columns(j, _):
            sk[j] = jnp.transpose(jnp.broadcast_to(segs[j], (HD, L)))
            return 0
        lax.fori_loop(0, 2 * NX, seg_columns, 0)
    tiles = [slice(b, b + HL) for b in range(0, L, HL)]

    def q_block(xx):
        return 2 * xx + lax.rem(k + xx, 2)

    def local(xx):
        return (x == xx) & (xodd == 0)

    def scores(xx, j, n, rows, diag):
        s = lax.dot_general(kg[j, 0:n, :], qg[xx, rows, :], (((1,), (1,)), ((), ())), preferred_element_type=F32)
        ok = jnp.concatenate([sk[j, 0:n, :]] * (HL // HD), axis=1) == jnp.broadcast_to(segs[q_block(xx)][:, rows], (n, HL))
        if diag:
            qi = lax.broadcasted_iota(jnp.int32, (n, HL), 1) + rows.start
            ok = ok & (lax.broadcasted_iota(jnp.int32, (n, HL), 0) <= qi)
        return jnp.where(ok, s * SCALE, -jnp.inf)

    def update(xx, blocks):
        for rows in tiles:
            ss = [scores(xx, j, L, rows, False) for j in blocks]
            m = m_s[xx, :, rows]
            m_new = m
            for s in ss:
                m_new = jnp.maximum(m_new, jnp.max(s, axis=0, keepdims=True))
            alpha = jnp.exp2(m - m_new)
            l, o = l_s[xx, :, rows] * alpha, o_s[xx, :, rows] * alpha
            for j, s in zip(blocks, ss):
                p = jnp.exp2(s - m_new)
                l += jnp.sum(p, axis=0, keepdims=True)
                o += jnp.dot(vg[j], p.astype(BF), preferred_element_type=F32)
            m_s[xx, :, rows], l_s[xx, :, rows], o_s[xx, :, rows] = m_new, l, o

    def o_ret(xx):
        ocol = pl.ds(pl.multiple_of(s_me * F + x * HD, HD), HD)
        return rcopy(obuf.at[xx], og.at[:, ocol], o_send.at[xx], o_recv.at[x], {"cp": q_block(xx)}), ocol

    def finish(xx):
        obuf[xx] = jnp.transpose(o_s[xx] / l_s[xx]).astype(BF)
        ret, ocol = o_ret(xx)

        @pl.when(local(xx))
        def _():
            og[:, ocol] = obuf[xx]

        pl.when(jnp.logical_not(local(xx)))(ret.start)

    def q_in(a):
        xx = mod(x + a, NX)
        return rcopy(qg.at[xx], qg.at[xx], q_send.at[3], q_recv.at[xx], partner)

    def attend_own(a):
        xx = mod(x + a, NX)
        c_q = q_block(xx)
        for rows in tiles:
            s = scores(xx, c_q, rows.stop, rows, True)
            m = jnp.max(s, axis=0, keepdims=True)
            p = jnp.exp2(s - m)
            m_s[xx, :, rows] = m
            l_s[xx, :, rows] = jnp.sum(p, axis=0, keepdims=True)
            o_s[xx, :, rows] = jnp.dot(vg[c_q, :, 0:rows.stop], p.astype(BF), preferred_element_type=F32)

    def attend_before(xx):
        def chip_step(i, _):
            update(xx, [2 * i, 2 * i + 1])
            return 0
        lax.fori_loop(0, xx, chip_step, 0)
        finish(xx)

    def wait_o():
        for h in range(NX):
            o_in = rcopy(obuf.at[0], og.at[:, pl.ds(pl.multiple_of(s_me * F + h * HD, HD), HD)], o_send.at[0], o_recv.at[h], partner)
            pl.when(jnp.logical_not((x == h) & (xodd == 0)))(o_in.wait_recv)

    with jax.named_scope("own0"):
        kv_partner(0, kg)
        kv_partner(1, vg)
        pl.when(xodd == 1)(q_in(0).wait_recv)
        attend_own(0)
    with jax.named_scope("fwd_v"):
        kv_forward(1, vg)

    with jax.named_scope("fin_kv"):
        kv_finish(0, kg)
        kv_finish(1, vg)
    with jax.named_scope("own1"):
        q_in(1).wait_recv()
        q_in(3).wait_recv()
        wx_start()
        attend_own(1)
        attend_own(3)
        wx_second()
    with jax.named_scope("own2"):
        q_in(2).wait_recv()
        attend_own(2)
        for xx in (1 - k, 3 - k):
            update(xx, [2 * xx])
    for a in (2, 3, 1, 0):
        with jax.named_scope("attn%d" % a):
            attend_before(mod(x + a, NX))
    def row_ds(r):
        return pl.ds(ROWS[r][0], ROWS[r][1])

    def o_copy(r, idx, zz, e, dev):
        s = zz * 2 + lax.rem(yb + e, 2)
        ref = og.at[row_ds(r), pl.ds(pl.multiple_of(s * F, F), F)]
        return rcopy(ref, ref, a_send, a_recv.at[r, idx], dev)

    def o_send_z(r, e):
        d = O_DIR[r]
        go(o_copy(r, 1 + 3 * e, z, e, tpdev(mod(z + d, NX), y)))
        go(o_copy(r, 2 + 3 * e, z, e, tpdev(mod(z + NX - d, NX), y)))

    pair = tpdev(z, yh * 2 + 1 - yb)
    o_seen = []

    def ostart(r):
        if not o_seen:
            o_seen.append(r)
            with jax.named_scope("wait_o"):
                wait_o()
        go(o_copy(r, 0, z, 0, pair))
        o_send_z(r, 0)
        if len(o_seen) == 1:
            o_seen.append(r)
            wx_relay()
            w_forward((0, 1, 3))

    def o_forward(r, e):
        d = O_DIR[r]
        zz = mod(z + NX - d, NX)
        o_copy(r, 1 + 3 * e, zz, e, partner).wait_recv()
        go(o_copy(r, 3 + 3 * e, zz, e, tpdev(mod(z + d, NX), y)))

    def o_pair(r, idx, new, zz):
        o_copy(r, idx, zz, 0, partner).wait_recv()
        go(o_copy(r, new, zz, 0, pair))

    def opair(r):
        if O_FIRST[r] == 0:
            o_pair(r, 2, 5, mod(z + O_DIR[r], NX))
            return
        o_copy(r, 0, z, 1, partner).wait_recv()
        o_send_z(r, 1)

    def ofw0(r):
        o_forward(r, 0)
        if O_FIRST[r] == 0:
            go(o_copy(r, 4, mod(z + NX - O_DIR[r], NX), 0, pair))

    def ofw1(r):
        if O_FIRST[r] == 0:
            o_pair(r, 3, 6, mod(z + 2, NX))
            return
        o_forward(r, 1)

    def o_rest(r):
        d = O_DIR[r]
        if O_FIRST[r] == 0:
            for idx, zz in ((0, z), (4, mod(z + NX - d, NX)), (5, mod(z + d, NX)), (6, mod(z + 2, NX))):
                o_copy(r, idx, zz, 1, partner).wait_recv()
            return
        for e in range(2):
            o_copy(r, 2 + 3 * e, mod(z + d, NX), e, partner).wait_recv()
            o_copy(r, 3 + 3 * e, mod(z + 2, NX), e, partner).wait_recv()

    def matmul(r, half):
        out = psend if half == 0 else pown
        hh = (1 - yh) if half == 0 else yh
        a, n = ROWS[r]
        for b in range(2):
            cols = pl.ds(pl.multiple_of(hh * F + b * 256, 256), 256)
            out[a:a + n, b * 256:(b + 1) * 256] = jnp.dot(og[a:a + n, :], wt[:, :, cols].reshape(8 * F, 256), preferred_element_type=F32)

    def rs_copy(r):
        return rcopy(psend.at[row_ds(r), :], rsb.at[row_ds(r), :], r_send, r_recv.at[r], tpdev(z, 3 - y))

    def mm0(r):
        o_rest(r)
        if r == first_mm:
            with jax.named_scope("w_done"):
                w_done()
        matmul(r, 0)
        go(rs_copy(r))

    def y_pos(r, a, b):
        if Y_ORDER[r] == 0:
            return mod(z + a, NX), mod(y + b, NX)
        return mod(z + b, NX), mod(y + a, NX)

    def y_ref(r, pos):
        return yg.at[row_ds(r), pl.ds(pl.multiple_of(piece_of(*pos) * F, F), F)]

    def y_copy(r, idx, pos, dev):
        ref = y_ref(r, pos)
        return rcopy(ref, ref, y_send, y_recv.at[r, idx], dev)

    def y_second(r, j, a):
        d2 = Y_DIR[r][1]
        pos = y_pos(r, a, 0)
        go(y_copy(r, 3 + 3 * j, pos, tpdev(*y_pos(r, 0, d2))))
        go(y_copy(r, 4 + 3 * j, pos, tpdev(*y_pos(r, 0, NX - d2))))

    def yst(r):
        rs_copy(r).wait_recv()
        a, n = ROWS[r]
        yg[a:a + n, pl.ds(pl.multiple_of(piece_of(z, y) * F, F), F)] = (pown[a:a + n, :] + rsb[a:a + n, :]).astype(BF)
        d = Y_DIR[r][0]
        pos = y_pos(r, 0, 0)
        go(y_copy(r, 0, pos, tpdev(*y_pos(r, d, 0))))
        go(y_copy(r, 1, pos, tpdev(*y_pos(r, NX - d, 0))))
        y_second(r, 0, 0)

    def ym0(r):
        d = Y_DIR[r][0]
        pos = y_pos(r, NX - d, 0)
        y_copy(r, 0, pos, partner).wait_recv()
        go(y_copy(r, 2, pos, tpdev(*y_pos(r, d, 0))))
        y_second(r, 1, NX - d)

    def ym1(r):
        d = Y_DIR[r][0]
        y_copy(r, 1, y_pos(r, d, 0), partner).wait_recv()
        y_second(r, 2, d)

    def ym2(r):
        y_copy(r, 2, y_pos(r, 2, 0), partner).wait_recv()
        y_second(r, 3, 2)

    def y_offs(r):
        d = Y_DIR[r][0]
        return (0, NX - d, d, 2)

    def yf(r, j):
        d2 = Y_DIR[r][1]
        pos = y_pos(r, y_offs(r)[j], NX - d2)
        y_copy(r, 3 + 3 * j, pos, partner).wait_recv()
        go(y_copy(r, 5 + 3 * j, pos, tpdev(*y_pos(r, 0, d2))))

    def ye(r):
        d2 = Y_DIR[r][1]
        for j, a in enumerate(y_offs(r)):
            y_copy(r, 4 + 3 * j, y_pos(r, a, d2), partner).wait_recv()
            y_copy(r, 5 + 3 * j, y_pos(r, a, 2), partner).wait_recv()

    steps = dict(ostart=ostart, opair=opair, ofw0=ofw0, ofw1=ofw1, mm0=mm0,
                 mm1=lambda r: matmul(r, 1), wxl=wx_last, yst=yst, ym0=ym0, ym1=ym1, ym2=ym2, yf=yf, ye=ye)
    first_mm = [a[1] for a in ORDER if a[0] == "mm0"][0]
    def drain(ref, sem):
        rcopy(ref, ref, sem, r_recv.at[0], partner).wait_send()

    def drain_early():
        drain(segs.at[pl.ds(0, 7)], sg_send)
        drain(kg.at[pl.ds(0, 7)], kv_send.at[0])
        drain(vg.at[pl.ds(0, 7)], kv_send.at[1])
        drain(wt.at[pl.ds(0, 7), pl.ds(0, HR), :], ws_send)
        drain(wt.at[pl.ds(0, 7), pl.ds(0, U), :], sh_send)
        drain(wt.at[pl.ds(0, 7), pl.ds(0, HR), :], wf_send)
        drain(wt.at[:, pl.ds(0, 7 * U), :], wx_send)
        for cp_ in sends:
            cp_.wait_send()

        @pl.when(xodd == 1)
        def _():
            q_d2d.wait_send()

        for xx in range(NX):
            pl.when(jnp.logical_not(local(xx)))(o_ret(xx)[0].wait_send)

    last_y = [a[1] for a in ORDER if a[0] == "yst"][-1]
    for name, *args in ORDER:
        with jax.named_scope(name + "_".join(str(a) for a in args)):
            steps[name](*args)
        if name == "yst" and args[0] == last_y:
            drain_early()

    drain(psend, r_send)
    drain(og.at[:, pl.ds(0, 7 * F)], a_send)
    drain(yg.at[:, pl.ds(0, 15 * F)], y_send)


def solution(mesh):
    def body(x, doc, wq, wk, wv, wo):
        seg = doc.reshape(1, L)
        dma = pltpu.SemaphoreType.DMA
        any_ = pl.BlockSpec(memory_space=pl.ANY)
        return pl.pallas_call(
            kernel,
            out_shape=pltpu.VMEM((L, D), BF),
            in_specs=[any_] * 6,
            out_specs=pl.BlockSpec(memory_space=pltpu.VMEM),
            scratch_shapes=[
                pltpu.VMEM((NKC, L, KC), BF), pltpu.VMEM((NB, KC, F), BF), pltpu.VMEM((L, F), F32),
                pltpu.VMEM((4, L, HD), BF), pltpu.VMEM((4, HD, L), BF), pltpu.VMEM((4, L, HD), BF),
                pltpu.VMEM((8, L, HD), BF), pltpu.VMEM((8, HD, L), BF), pltpu.VMEM((4, L, HD), BF), pltpu.VMEM((4, L, HD), BF),
                pltpu.VMEM((L, 8 * F), BF), pltpu.VMEM((8, F, 1024), BF),
                pltpu.VMEM((L, F), F32), pltpu.VMEM((L, F), F32), pltpu.VMEM((L, F), F32),
                pltpu.VMEM((8, 1, L), jnp.int32), pltpu.VMEM((8, L, HD), jnp.int32),
                pltpu.VMEM((NX, 1, L), F32), pltpu.VMEM((NX, 1, L), F32), pltpu.VMEM((NX, HD, L), F32),
                dma((NKC,)), dma((NB,)), dma((2,)), dma, dma((7,)), dma, dma((7,)), dma, dma((7,)), dma, dma((10,)),
                dma((2,)), dma((2, 4)), dma((2, 3)), dma((4,)), dma((4,)), dma((4,)), dma((4,)),
                dma, dma((7,)), dma, dma, dma((R, 7)), dma, dma((R,)), dma, dma((R, 15)),
            ],
            compiler_params=pltpu.CompilerParams(collective_id=0, has_side_effects=True, vmem_limit_bytes=50 * 1024 * 1024),
        )(x, seg, wq, wk, wv, wo)

    return jax.shard_map(body, mesh=mesh, in_specs=(P(('dp', 'cp'), None), P(('dp', 'cp')), P(None, 'tp'), P(None, 'tp'), P(None, 'tp'), P('tp', None)), out_specs=P(('dp', 'cp'), None), check_vma=False)
```
